32 devices in a mesh: groups: 2 (over y), blk: 4 (over z), tok: 4 (over x, core).
Axes of the slice: x: 2, y: 2, z: 4, core: 2. Of those that a mesh axis runs over, the one named last changes fastest.
Arguments:
- tokens: bfloat16 [2048, 3584], P(('groups', 'blk', 'tok')), parts along dimension 0, may hold values from -6 to 6
- expert_ids: int32 [2048, 1], P(('groups', 'blk', 'tok')), parts along dimension 0, may hold values from 0 to 1; in each aligned block of 256 rows (0 to 255, 256 to 511, ...) at most 192 rows name the same one
- gate_values: float32 [2048, 1], P(('groups', 'blk', 'tok')), parts along dimension 0, may hold values from 0.2 to 1
- w_gate: bfloat16 [2, 3584, 1024], P(None, 'blk', 'tok'), may hold values from -0.09375 to 0.09375
- w_up: bfloat16 [2, 3584, 1024], P(None, 'blk', 'tok'), may hold values from -0.09375 to 0.09375
- w_down: bfloat16 [2, 1024, 3584], P(None, 'tok', 'blk'), may hold values from -0.1875 to 0.1875
Outputs:
- mixed: bfloat16 [2048, 3584], P(('groups', 'blk', 'tok')), parts along dimension 0
The draws below stay inside these ranges and needn't reach their ends.
There are 2 independent parts, one for each index of `groups`. The reference program is written for one: setup_inputs(seed, part) draws one part's arguments, and reference() takes and returns one part's arrays. A program takes and returns all parts, laid end to end along the dimension named above; an argument that names none is the same for every part. Nothing has to cross between parts.
Inputs may be any that keep to these rules, and one draw needn't show every extreme that they name: `expert_ids`: in each aligned block of 256 rows (the tokens of one index of blk), no expert is named by more than 192 rows, and in every draw some expert reaches 192 in some block.
All inputs are finite; a program needn't handle non-finite values.
Results may differ from the reference program's by a relative error of at most 0.005.
Values may be sent and summed in bfloat16 or wider, within the bound.
A program may use at most 64 MiB of HBM per device.

```python
import math
import jax
import jax.numpy as jnp
import numpy as np
from jax import lax

D = 3584
FF = 1024
EXPERTS = 2
TOPK = 1
GROUP = 256
CAP = 192
TOKENS = 1024


def steps_of(key, shape, cuts, least, high):
    def one(axis_at, shards_of):
        heights = jax.random.uniform(jax.random.fold_in(jax.random.fold_in(key, 6), axis_at), (shards_of,), jnp.float32, least / len(cuts), high / len(cuts))
        return jnp.repeat(jnp.exp(heights), shape[axis_at] // shards_of).reshape((-1,) + (1,) * (len(shape) - axis_at - 1))

    gain = one(*cuts[0])
    for cut in cuts[1:]:
        gain = gain * one(*cut)
    return gain


def assign_block(stream_key, own, number, rows, amount, top, reach, slope):
    sequence = jax.random.permutation(stream_key, amount)
    crowded, ordinary = shares(amount, rows * top, reach, slope, True), shares(amount, rows * top, reach, slope, False)
    places = jnp.arange(amount)

    def named(tallies, turn):
        used = int((tallies > 0).sum())
        fixed = max(1, used // 4)
        moved = fixed + (places - fixed + turn * (used - fixed)) % max(1, amount - fixed)
        return jnp.zeros((amount,), jnp.int32).at[sequence[jnp.where(places < fixed, places, moved)]].set(jnp.asarray(tallies, jnp.int32))

    tallies = jnp.where(number % 4 == 0, named(crowded, number // 4), named(ordinary, number - number // 4 - 1))
    mixed = jax.random.permutation(jax.random.fold_in(own, 3), amount)
    source_of, taker = mixed[0:amount // 2 * 2:2], mixed[1:amount // 2 * 2:2]
    margin = jnp.minimum(tallies[source_of] - 1, reach - tallies[taker]) // 2
    margin = jnp.where((source_of == sequence[0]) | (taker == sequence[0]) | (tallies[taker] == 0), 0, jnp.maximum(margin, 0))
    moved = jax.random.randint(jax.random.fold_in(own, 4), (amount // 2,), 0, 1 << 20) % (margin + 1)
    tallies = tallies.at[source_of].add(-moved).at[taker].add(moved)
    labels = jnp.searchsorted(jnp.cumsum(tallies), jnp.arange(rows * top), side="right").astype(jnp.int32)
    listing = labels.reshape(top, rows).T
    listing = listing[jax.random.permutation(jax.random.fold_in(own, 1), rows)]
    turn = jax.random.randint(jax.random.fold_in(own, 2), (rows, 1), 0, top)
    return jnp.take_along_axis(listing, (jnp.arange(top)[None, :] + turn) % top, axis=1)


def shares(amount, total, most, lean, full):
    portions = [(1 << 20) // math.isqrt(rank ** lean) + 1 for rank in range(1, amount + 1)]
    largest = most if full else min(most, max(-(-total // amount), total * portions[0] // sum(portions)))
    least = 1 if total - largest >= amount - 1 else 0
    given, spare = [largest] + [least] * (amount - 1), total - largest - least * (amount - 1)
    while spare > 0:
        candidates = [i for i in range(1, amount) if given[i] < largest] or [i for i in range(1, amount) if given[i] < most]
        whole, budget = sum([portions[i] for i in candidates]), spare
        for i in candidates:
            extra = min(most - given[i], max(1, budget * portions[i] // whole), spare)
            given[i] = given[i] + extra
            spare = spare - extra
    return np.array(given)


def gaussian(stream_key, dims, width, limit, cuts=(), kind=jnp.bfloat16):
    drawn = jax.random.normal(stream_key, dims, jnp.float32) * width
    if len(cuts) > 0:
        drawn = steps_of(stream_key, dims, cuts, -0.22, 0.18) * drawn
    return jnp.clip(drawn, min=-limit, max=limit).astype(kind)


def setup_inputs(seed: int = 0, part: int = 0) -> dict:
    streams_of = jax.random.split(jax.random.key(seed), 7)
    own_keys = jax.random.split(jax.random.fold_in(streams_of[6], part), 7)
    tokens = gaussian(own_keys[0], (TOKENS, D), 1.0, 6.0, ((0, 16),))
    expert_ids_keys = jax.random.split(jax.random.fold_in(own_keys[1], 1), TOKENS // GROUP)
    expert_ids_turns = jax.random.permutation(jax.random.fold_in(own_keys[1], 3), TOKENS // GROUP)
    expert_ids = jax.vmap(lambda own, number: assign_block(jax.random.fold_in(own_keys[1], 2), own, number, GROUP, EXPERTS, TOPK, CAP, 2))(expert_ids_keys, expert_ids_turns).reshape((TOKENS, TOPK))
    gate_values = jnp.clip(0.2 + 0.8 * jax.random.uniform(own_keys[2], (TOKENS, TOPK), jnp.float32) ** steps_of(own_keys[2], (TOKENS, TOPK), ((0, 16),), -0.2, 0.2), 0.2, 1.0)
    w_gate = gaussian(streams_of[3], (EXPERTS, D, FF), D ** -0.5, 0.09375, ((1, 4), (2, 4)))
    w_up = gaussian(streams_of[4], (EXPERTS, D, FF), D ** -0.5, 0.09375, ((1, 4), (2, 4)))
    w_down = gaussian(streams_of[5], (EXPERTS, FF, D), FF ** -0.5, 0.1875, ((1, 4), (2, 4)))
    return {"tokens": tokens, "expert_ids": expert_ids, "gate_values": gate_values, "w_gate": w_gate, "w_up": w_up, "w_down": w_down}


block_rows = 512


def expert_block(token_block, gate_weight, up_weight, down_weight):
    gate = jnp.dot(token_block, gate_weight, preferred_element_type=jnp.float32)
    up = jnp.dot(token_block, up_weight, preferred_element_type=jnp.float32)
    hidden = (jax.nn.silu(gate) * up).astype(jnp.bfloat16)
    return jnp.dot(hidden, down_weight, preferred_element_type=jnp.float32)


def reference(tokens, expert_ids, gate_values, w_gate, w_up, w_down):
    count_tokens = tokens.shape[0]
    routes = expert_ids[:, 0].astype(jnp.int32)
    onehot = (routes[:, None] == jnp.arange(EXPERTS, dtype=jnp.int32)[None, :]).astype(jnp.int32)
    slot_rank = jnp.sum((jnp.cumsum(onehot, axis=0) - onehot) * onehot, axis=1).astype(jnp.int32)
    counts = jnp.sum(onehot, axis=0).astype(jnp.int32)
    padded = ((counts + block_rows - 1) // block_rows) * block_rows
    starts = (jnp.cumsum(padded) - padded).astype(jnp.int32)
    destination = (jnp.take(starts, routes) + slot_rank).astype(jnp.int32)
    num_blocks = (count_tokens + block_rows - 1) // block_rows + EXPERTS
    total_slots = num_blocks * block_rows
    slot_token = jnp.zeros((total_slots,), jnp.int32).at[destination].set(jnp.arange(count_tokens, dtype=jnp.int32))
    block_start = jnp.arange(num_blocks, dtype=jnp.int32) * block_rows
    block_expert = jnp.sum((starts[None, :] <= block_start[:, None]).astype(jnp.int32), axis=1) - 1
    block_expert = jnp.clip(block_expert, 0, EXPERTS - 1).astype(jnp.int32)

    def run_block(args):
        indices, expert = args
        token_block = jnp.take(tokens, indices, axis=0)
        return expert_block(token_block, w_gate[expert], w_up[expert], w_down[expert])

    outputs = lax.map(run_block, (slot_token.reshape(num_blocks, block_rows), block_expert))
    flat_rows = outputs.reshape(total_slots, tokens.shape[1])
    expert_out = jnp.take(flat_rows, destination, axis=0)
    return (gate_values[:, 0:1] * expert_out).astype(jnp.bfloat16)
```

```python
import functools

import jax
import jax.numpy as jnp
from jax import lax
from jax.experimental import pallas as pl
from jax.experimental.pallas import tpu as pltpu
from jax.sharding import PartitionSpec as P

LANES = 128
SUBLANES = 8
WAVES = 2
ORDER = (
    ("Z", 0, 3), ("S", 1, 0), ("Z", 0, 1), ("S", 0, 0), ("Z", 0, 2), ("S", 0, 3),
    ("Z", 1, 3), ("S", 0, 2), ("Z", 1, 2), ("P", 0, 0), ("P", 0, 3), ("S", 0, 1),
    ("Z", 1, 1), ("C", 0, 0), ("C", 0, 3), ("P", 0, 2), ("S", 1, 3), ("C", 0, 2),
    ("S", 1, 2), ("P", 1, 3), ("P", 1, 0), ("P", 0, 1), ("R", 0, 2), ("C", 1, 3),
    ("S", 1, 1), ("P", 1, 2), ("C", 1, 2), ("C", 0, 1), ("R", 0, 3), ("R", 1, 2),
    ("C", 1, 0), ("R", 1, 3), ("P", 1, 1), ("C", 1, 1), ("A", 0, 0), ("A", 1, 0),
    ("H", 0, 3), ("E", 0, 0), ("E", 1, 0), ("H", 0, 2), ("E", 0, 2), ("H", 1, 3),
    ("E", 0, 3), ("X", 0, 2), ("E", 0, 1), ("X", 0, 3), ("X", 1, 0), ("H", 1, 2),
    ("E", 1, 1), ("E", 1, 3), ("F", 0, 2), ("X", 1, 3), ("F", 0, 3), ("E", 1, 2),
    ("X", 1, 1), ("X", 0, 1), ("X", 1, 2), ("X", 0, 0), ("F", 1, 3), ("F", 1, 1),
    ("F", 1, 0), ("F", 1, 2), ("F", 0, 0), ("F", 0, 1),
)


def gathered_body(tokens, expert_ids, gate_values, w_gate, w_up, w_down):
    group_rows = lax.all_gather(tokens, "tok", axis=0, tiled=True)
    group_routes = lax.all_gather(expert_ids, "tok", axis=0, tiled=True)[:, 0]
    experts = w_gate.shape[0]
    count_rows = group_rows.shape[0]
    capacity = 3 * count_rows // 4
    expert_range = jnp.arange(experts, dtype=jnp.int32)
    onehot = (group_routes[:, None] == expert_range[None, :]).astype(jnp.int32)
    slot_rank = jnp.sum((jnp.cumsum(onehot, axis=0) - onehot) * onehot, axis=1)
    expert_match = group_routes[None, None, :] == expert_range[:, None, None]
    slot_match = slot_rank[None, None, :] == jnp.arange(capacity, dtype=jnp.int32)[None, :, None]
    dispatch = (expert_match & slot_match).astype(jnp.bfloat16)
    slots = jnp.einsum(
        "esg,gd->esd", dispatch, group_rows, preferred_element_type=jnp.float32
    ).astype(jnp.bfloat16)

    def add_part(weights):
        return jnp.einsum("esd,edf->esf", slots, weights, preferred_element_type=jnp.float32)

    gate_sum = add_part(lax.all_gather(w_gate, "blk", axis=1, tiled=True))
    up_sum = add_part(lax.all_gather(w_up, "blk", axis=1, tiled=True))
    hidden = (jax.nn.silu(gate_sum) * up_sum).astype(jnp.bfloat16)
    slot_out = jnp.einsum(
        "esf,efd->esd",
        hidden,
        lax.all_gather(w_down, "blk", axis=2, tiled=True),
        preferred_element_type=jnp.float32,
    )
    flat_rows = slot_out.reshape(experts * capacity, slot_out.shape[2])
    position = group_routes * capacity + slot_rank
    partial_value = jnp.take(flat_rows, position, axis=0)
    summed = lax.psum_scatter(partial_value, "tok", scatter_dimension=0, tiled=True)
    return (gate_values * summed).astype(jnp.bfloat16)


def kernel(
    nb, nt, tok_hbm, ids_hbm, values_hbm, wg_hbm, wu_hbm, wd_hbm, out_ref,
    tok, ids, values, meta, wg, wu, wd, routes, scales, xs, part, part_send, part_recv, hid, ys, ycore,
    yx_send, yx_recv, fin_send,
    local_sem, send_sem, far, m_recv, z_recv, x_recv, c_recv, p_recv, h_recv, y_recv, yx_sem, o_recv,
):
    g, b, t = lax.axis_index("groups"), lax.axis_index("blk"), lax.axis_index("tok")
    all_rows, width = tok.shape[0], xs.shape[4]
    rows = all_rows // WAVES
    block = nt * rows
    experts, ff = wg.shape[0], wg.shape[2]
    f32, bf16 = jnp.float32, jnp.bfloat16
    pair = t + 1 - 2 * lax.rem(t, 2)
    across = lax.rem(t + 2, nt)
    across_pair = lax.rem(pair + 2, nt)
    outer = lax.rem((b + 1) // 2 + 1, 2) == 1
    inner = jnp.logical_not(outer)

    low, high = lax.rem(b, 2), b // 2
    blocks = [b, 2 * high + 1 - low, 2 * (1 - high) + low, 2 * (1 - high) + 1 - low]

    def blk(k):
        return blocks[k]

    def cols(index):
        return pl.ds(pl.multiple_of(index * width, LANES), width)

    def of_wave(w):
        return pl.ds(w * rows, rows)

    def noted(block_at, token_at):
        return block_at * nt + token_at

    def owned(index):
        return pl.ds(pl.multiple_of(index * rows, SUBLANES), rows)

    def remote(src, dst, kind, recv, to_b, to_t):
        pltpu.make_async_remote_copy(
            src_ref=src, dst_ref=dst, send_sem=send_sem.at[kind], recv_sem=recv,
            device_id=(g, to_b, to_t), device_id_type=pl.DeviceIdType.MESH,
        ).start()

    def arrived(dst, recv):
        pltpu.make_async_copy(dst, dst, recv).wait()

    def signal(sem, to_b, to_t):
        pl.semaphore_signal(sem, inc=1, device_id=(g, to_b, to_t), device_id_type=pl.DeviceIdType.MESH)

    own = [
        pltpu.make_async_copy(tok_hbm.at[of_wave(w), cols(b)], xs.at[w, b, t], local_sem.at[4])
        for w in range(WAVES)
    ]
    local = [
        pltpu.make_async_copy(tok_hbm, tok, local_sem.at[0]),
        pltpu.make_async_copy(wg_hbm, wg, local_sem.at[1]),
        pltpu.make_async_copy(wu_hbm, wu, local_sem.at[2]),
        pltpu.make_async_copy(wd_hbm, wd, local_sem.at[3]),
    ]
    notes = [
        pltpu.make_async_copy(ids_hbm, ids, local_sem.at[5]),
        pltpu.make_async_copy(values_hbm, values, local_sem.at[6]),
    ]
    barrier = pltpu.get_barrier_semaphore()
    signal(barrier, b, pair)
    signal(barrier, b, across)
    signal(barrier, blk(1), t)

    @pl.when(inner)
    def _():
        signal(barrier, blk(3), t)

    for copy in notes + local[:1] + own + local[1:]:
        copy.start()
    for copy in notes:
        copy.wait()
    meta[noted(b, t)] = jnp.zeros((SUBLANES, LANES), f32)
    meta[noted(b, t), 0:1, :all_rows] = ids[...].astype(f32)
    meta[noted(b, t), 1:2, :all_rows] = values[...]

    @pl.when(inner)
    def _():
        pl.semaphore_wait(barrier, 4)
        signal(far.at[0], blk(1), t)
        signal(far.at[0], blk(3), t)

    @pl.when(outer)
    def _():
        pl.semaphore_wait(barrier, 3)

    local[0].wait()
    arrived(fin_send.at[:, 0], local_sem.at[4])

    def far_known():
        pl.semaphore_wait(far.at[0], 1)

        @pl.when(inner)
        def _():
            signal(far.at[1], blk(1), t)

    def far_end():
        @pl.when(outer)
        def _():
            pl.semaphore_wait(far.at[1], 1)

    ready = {"weights": False, "down": False, "far": False, "end": False}

    def launch(w, k):
        if k == 2 and not ready["far"]:
            far_known()
            ready["far"] = True
        if k == 3 and not ready["end"]:
            far_end()
            ready["end"] = True
        if w == 0:
            note = meta.at[noted(b, t)]
            remote(note, note, 9, m_recv.at[0, k], blk(k), t)
        remote(tok.at[of_wave(w), cols(blk(k))], xs.at[w, b, t], 0, z_recv.at[w, k - 1], blk(k), t)

    def spread(w, k):
        source = blk(k)
        mine = xs.at[w, source, t]
        if w == 0:
            note = meta.at[noted(source, t)]
            if k:
                arrived(note, m_recv.at[0, k])
            remote(note, note, 9, m_recv.at[1, k], b, across)
            remote(note, note, 9, m_recv.at[2, k], b, pair)
        if k:
            arrived(mine, z_recv.at[w, k - 1])
        remote(mine, mine, 1, x_recv.at[w, k], b, across)
        remote(mine, mine, 2, c_recv.at[w, k], b, pair)

    def pass_on(w, k):
        source = blk(k)
        theirs = xs.at[w, source, across]
        if w == 0:
            note = meta.at[noted(source, across)]
            arrived(note, m_recv.at[1, k])
            remote(note, note, 9, m_recv.at[2, k], b, pair)
        arrived(theirs, x_recv.at[w, k])
        remote(theirs, theirs, 2, c_recv.at[w, k], b, pair)

    def wide(mask, size):
        return jnp.concatenate([mask] * (size // LANES), axis=1)

    def prepare(k):
        source = blk(k)
        arrived(meta.at[pl.ds(0, 2)], m_recv.at[2, k])
        turned = jnp.transpose(meta[pl.ds(source * nt, nt)].reshape(nt * SUBLANES, LANES))
        for row, out in ((0, routes),) if k else ((0, routes), (1, scales)):
            for w in range(WAVES):
                column = jnp.concatenate(
                    [turned[w * rows:(w + 1) * rows, SUBLANES * i + row:SUBLANES * i + row + 1] for i in range(nt)],
                    axis=0,
                )
                out[w, k] = jnp.broadcast_to(column, (block, LANES))

    def contract(w, k):
        source = blk(k)
        if w == 0:
            prepare(k)
        arrived(xs.at[w, source, pl.ds(0, 2)], c_recv.at[w, k])
        if not ready["weights"]:
            local[1].wait()
            local[2].wait()
            ready["weights"] = True
        chosen = wide(routes[w, k], ff)
        x = xs[w, source].reshape(block, width)
        for at, weights in ((0, wg), (ff, wu)):
            total = None
            for e in range(experts):
                value = jnp.dot(x, weights[e], preferred_element_type=f32)
                total = value if e == 0 else jnp.where(chosen == e, value, total)
            part[w, k, :, at:at + ff] = total
            if k:
                part_send[w, k, :, at:at + ff] = total.astype(bf16)
        if k == 1:
            remote(part_send.at[w, 1], part_recv.at[w, 0], 6, p_recv.at[w, 0], blk(1), t)
        elif k:
            @pl.when(outer)
            def _():
                remote(part_send.at[w, k], part_recv.at[w, 5 - k], 6, p_recv.at[w, 5 - k], blk(1), t)

    def relay(w, k):
        @pl.when(inner)
        def _():
            arrived(part_recv.at[w, k], p_recv.at[w, k])
            part_send[w, k] = (part[w, k] + part_recv[w, k].astype(f32)).astype(bf16)
            remote(part_send.at[w, k], part_recv.at[w, 1], 6, p_recv.at[w, 1], blk(k), t)

    def activate(w, k):
        total = part[w, 0]
        for slot in (0, 1):
            arrived(part_recv.at[w, slot], p_recv.at[w, slot])
            total = total + part_recv[w, slot].astype(f32)
        gate, up = total[:, :ff], total[:, ff:]
        hid[w, b] = (gate / (1.0 + jnp.exp(-gate)) * up * wide(scales[w, 0], ff)).astype(bf16)
        mine = hid.at[w, b]

        @pl.when(inner)
        def _():
            remote(mine, mine, 7, h_recv.at[w, 2], blk(3), t)

        remote(mine, mine, 7, h_recv.at[w, 0], blk(1), t)

        @pl.when(outer)
        def _():
            remote(mine, mine, 7, h_recv.at[w, 1], blk(2), t)

    def forward(w, k):
        @pl.when(inner)
        def _():
            source = blk(k)
            theirs = hid.at[w, source]
            arrived(theirs, h_recv.at[w, k - 1])
            if k == 1:
                remote(theirs, theirs, 8, h_recv.at[w, 1], blk(3), t)
            else:
                remote(theirs, theirs, 8, h_recv.at[w, 4 - k], blk(1), t)

    def expand(w, k):
        source = blk(k)
        if not ready["down"]:
            local[3].wait()
            ready["down"] = True
        if k:
            if k in (2, 3):
                @pl.when(outer)
                def _():
                    arrived(hid.at[w, source], h_recv.at[w, k - 1])
            else:
                arrived(hid.at[w, source], h_recv.at[w, k - 1])
        chosen = wide(routes[w, k], ff)
        h = hid[w, source].astype(f32)
        routed = jnp.concatenate([jnp.where(chosen == e, h, 0.0).astype(bf16) for e in range(experts)], axis=1)
        ys[w, k] = jnp.dot(routed, wd[...].reshape(experts * ff, width), preferred_element_type=f32)
        for j, place in ((1, across_pair), (0, pair)):
            remote(ys.at[w, k, owned(place)], ycore.at[w, k, j], 3, y_recv.at[w, k], b, pair)

    def exchange(w, k):
        arrived(ycore.at[w, k], y_recv.at[w, k])
        yx_send[w, k] = (ys[w, k, owned(across), :] + ycore[w, k, 1]).astype(bf16)
        remote(yx_send.at[w, k], yx_recv.at[w, k], 4, yx_sem.at[w, k], b, across)

    def finish(w, k):
        total = ys[w, k, owned(t), :] + ycore[w, k, 0]
        arrived(yx_recv.at[w, k], yx_sem.at[w, k])
        total = total + yx_recv[w, k].astype(f32)
        if k:
            fin_send[w, k] = total.astype(bf16)
            remote(fin_send.at[w, k], out_ref.at[of_wave(w), cols(b)], 5, o_recv.at[0], blk(k), t)
        else:
            out_ref[of_wave(w), cols(b)] = total.astype(bf16)

    steps = {
        "Z": launch, "S": spread, "P": pass_on, "C": contract, "R": relay,
        "A": activate, "H": forward, "E": expand, "X": exchange, "F": finish,
    }
    for name, w, k in ORDER:
        steps[name](w, k)

    others = fin_send.at[:, pl.ds(1, nb - 1)]
    arrived(others, o_recv.at[0])
    for kind, ref in (
        (0, others), (1, yx_send), (2, xs.at[:, :, pl.ds(0, 2)]), (3, ycore), (4, yx_send), (5, others),
        (6, part_send.at[:, pl.ds(1, nb - 1)]), (9, meta.at[pl.ds(0, nb * nt - 1)]),
    ):
        arrived(ref, send_sem.at[kind])

    @pl.when(inner)
    def _():
        arrived(hid.at[:, pl.ds(0, 2)], send_sem.at[7])
        arrived(hid.at[:, pl.ds(0, 2)], send_sem.at[8])

    @pl.when(outer)
    def _():
        arrived(hid.at[:, pl.ds(0, 2)], send_sem.at[7])


def stationary_body(nb, nt, tokens, expert_ids, gate_values, w_gate, w_up, w_down):
    rows, features = tokens.shape
    experts, width, ff = w_gate.shape
    f32, bf16 = jnp.float32, jnp.bfloat16
    wave_rows = rows // WAVES
    block = nt * wave_rows
    dma = pltpu.SemaphoreType.DMA
    vmem = pl.BlockSpec(memory_space=pltpu.VMEM)
    hbm = pl.BlockSpec(memory_space=pltpu.HBM)
    each = (WAVES, nb)
    return pl.pallas_call(
        functools.partial(kernel, nb, nt),
        out_shape=jax.ShapeDtypeStruct((rows, features), bf16),
        in_specs=[hbm] * 6,
        out_specs=vmem,
        scratch_shapes=[
            pltpu.VMEM((rows, features), bf16),
            pltpu.VMEM((1, rows), jnp.int32),
            pltpu.VMEM((1, rows), f32),
            pltpu.VMEM((nb * nt, SUBLANES, LANES), f32),
            pltpu.VMEM(w_gate.shape, bf16),
            pltpu.VMEM(w_up.shape, bf16),
            pltpu.VMEM(w_down.shape, bf16),
            pltpu.VMEM((*each, block, LANES), f32),
            pltpu.VMEM((WAVES, 1, block, LANES), f32),
            pltpu.VMEM((*each, nt, wave_rows, width), bf16),
            pltpu.VMEM((*each, block, 2 * ff), f32),
            pltpu.VMEM((*each, block, 2 * ff), bf16),
            pltpu.VMEM((*each, block, 2 * ff), bf16),
            pltpu.VMEM((*each, block, ff), bf16),
            pltpu.VMEM((*each, block, width), f32),
            pltpu.VMEM((*each, 2, wave_rows, width), f32),
            pltpu.VMEM((*each, wave_rows, width), bf16),
            pltpu.VMEM((*each, wave_rows, width), bf16),
            pltpu.VMEM((*each, wave_rows, width), bf16),
            dma((7,)),
            dma((10,)),
            pltpu.SemaphoreType.REGULAR((2,)),
            dma((3, nb)),
            dma((WAVES, nb - 1)), dma(each), dma(each), dma(each), dma((WAVES, nb - 1)), dma(each), dma(each), dma((1,)),
        ],
        compiler_params=pltpu.CompilerParams(
            collective_id=0, has_side_effects=True, vmem_limit_bytes=57000000,
        ),
    )(tokens, expert_ids.reshape(1, rows), gate_values.reshape(1, rows), w_gate, w_up, w_down)


def solution(mesh):
    nb, nt = mesh.shape["blk"], mesh.shape["tok"]

    def body(tokens, expert_ids, gate_values, w_gate, w_up, w_down):
        rows = tokens.shape[0]
        width, ff = w_gate.shape[1], w_gate.shape[2]
        fits = width % LANES == 0 and ff % LANES == 0 and rows % (16 * WAVES) == 0 and rows <= LANES
        if fits and nt == 4 and nb == 4:
            return stationary_body(nb, nt, tokens, expert_ids, gate_values, w_gate, w_up, w_down)
        return gathered_body(tokens, expert_ids, gate_values, w_gate, w_up, w_down)

    return jax.shard_map(
        body,
        mesh=mesh,
        in_specs=(
            P(("groups", "blk", "tok"), None),
            P(("groups", "blk", "tok"), None),
            P(("groups", "blk", "tok"), None),
            P(None, "blk", "tok"),
            P(None, "blk", "tok"),
            P(None, "tok", "blk"),
        ),
        out_specs=P(("groups", "blk", "tok"), None),
        check_vma=False,
    )
```

```python
import functools

import jax
import jax.numpy as jnp
from jax import lax
from jax.experimental import pallas as pl
from jax.experimental.pallas import tpu as pltpu
from jax.sharding import PartitionSpec as P

LANES = 128
SUBLANES = 8
WAVES = 2
ORDER = (
    ("Z", 0, 3), ("S", 1, 0), ("Z", 0, 1), ("S", 0, 0), ("Z", 0, 2), ("S", 0, 3),
    ("Z", 1, 3), ("S", 0, 2), ("Z", 1, 2), ("P", 0, 0), ("P", 0, 3), ("S", 0, 1),
    ("Z", 1, 1), ("C", 0, 0), ("C", 0, 3), ("P", 0, 2), ("S", 1, 3), ("C", 0, 2),
    ("S", 1, 2), ("P", 1, 3), ("P", 1, 0), ("P", 0, 1), ("R", 0, 2), ("C", 1, 3),
    ("S", 1, 1), ("P", 1, 2), ("C", 1, 2), ("C", 0, 1), ("R", 0, 3), ("R", 1, 2),
    ("C", 1, 0), ("R", 1, 3), ("P", 1, 1), ("C", 1, 1), ("A", 0, 0), ("A", 1, 0),
    ("H", 0, 3), ("E", 0, 0), ("E", 1, 0), ("H", 0, 2), ("E", 0, 2), ("H", 1, 3),
    ("E", 0, 3), ("X", 0, 2), ("E", 0, 1), ("X", 0, 3), ("X", 1, 0), ("H", 1, 2),
    ("E", 1, 1), ("E", 1, 3), ("F", 0, 2), ("X", 1, 3), ("F", 0, 3), ("E", 1, 2),
    ("X", 1, 1), ("X", 0, 1), ("X", 1, 2), ("X", 0, 0), ("F", 1, 3), ("F", 1, 1),
    ("F", 1, 0), ("F", 1, 2), ("F", 0, 0), ("F", 0, 1),
)


def gathered_body(tokens, expert_ids, gate_values, w_gate, w_up, w_down):
    group_rows = lax.all_gather(tokens, "tok", axis=0, tiled=True)
    group_routes = lax.all_gather(expert_ids, "tok", axis=0, tiled=True)[:, 0]
    experts = w_gate.shape[0]
    count_rows = group_rows.shape[0]
    capacity = 3 * count_rows // 4
    expert_range = jnp.arange(experts, dtype=jnp.int32)
    onehot = (group_routes[:, None] == expert_range[None, :]).astype(jnp.int32)
    slot_rank = jnp.sum((jnp.cumsum(onehot, axis=0) - onehot) * onehot, axis=1)
    expert_match = group_routes[None, None, :] == expert_range[:, None, None]
    slot_match = slot_rank[None, None, :] == jnp.arange(capacity, dtype=jnp.int32)[None, :, None]
    dispatch = (expert_match & slot_match).astype(jnp.bfloat16)
    slots = jnp.einsum(
        "esg,gd->esd", dispatch, group_rows, preferred_element_type=jnp.float32
    ).astype(jnp.bfloat16)

    def add_part(weights):
        return jnp.einsum("esd,edf->esf", slots, weights, preferred_element_type=jnp.float32)

    gate_sum = add_part(lax.all_gather(w_gate, "blk", axis=1, tiled=True))
    up_sum = add_part(lax.all_gather(w_up, "blk", axis=1, tiled=True))
    hidden = (jax.nn.silu(gate_sum) * up_sum).astype(jnp.bfloat16)
    slot_out = jnp.einsum(
        "esf,efd->esd",
        hidden,
        lax.all_gather(w_down, "blk", axis=2, tiled=True),
        preferred_element_type=jnp.float32,
    )
    flat_rows = slot_out.reshape(experts * capacity, slot_out.shape[2])
    position = group_routes * capacity + slot_rank
    partial_value = jnp.take(flat_rows, position, axis=0)
    summed = lax.psum_scatter(partial_value, "tok", scatter_dimension=0, tiled=True)
    return (gate_values * summed).astype(jnp.bfloat16)


def kernel(
    nb, nt, tok_hbm, ids_hbm, values_hbm, wg_hbm, wu_hbm, wd_hbm, out_ref,
    tok, ids, values, meta, wg, wu, wd, routes, scales, xs, part, part_send, part_recv, hid, ys, ycore,
    yx_send, yx_recv, fin_send,
    local_sem, send_sem, far, m_recv, z_recv, x_recv, c_recv, p_recv, h_recv, y_recv, yx_sem, o_recv,
):
    g, b, t = lax.axis_index("groups"), lax.axis_index("blk"), lax.axis_index("tok")
    all_rows, width = tok.shape[0], xs.shape[4]
    rows = all_rows // WAVES
    block = nt * rows
    experts, ff = wg.shape[0], wg.shape[2]
    f32, bf16 = jnp.float32, jnp.bfloat16
    pair = t + 1 - 2 * lax.rem(t, 2)
    across = lax.rem(t + 2, nt)
    across_pair = lax.rem(pair + 2, nt)
    outer = lax.rem((b + 1) // 2 + 1, 2) == 1
    inner = jnp.logical_not(outer)

    low, high = lax.rem(b, 2), b // 2
    blocks = [b, 2 * high + 1 - low, 2 * (1 - high) + low, 2 * (1 - high) + 1 - low]

    def blk(k):
        return blocks[k]

    def cols(index):
        return pl.ds(pl.multiple_of(index * width, LANES), width)

    def of_wave(w):
        return pl.ds(w * rows, rows)

    def noted(block_at, token_at):
        return block_at * nt + token_at

    def owned(index):
        return pl.ds(pl.multiple_of(index * rows, SUBLANES), rows)

    def remote(src, dst, kind, recv, to_b, to_t):
        pltpu.make_async_remote_copy(
            src_ref=src, dst_ref=dst, send_sem=send_sem.at[kind], recv_sem=recv,
            device_id=(g, to_b, to_t), device_id_type=pl.DeviceIdType.MESH,
        ).start()

    def arrived(dst, recv):
        pltpu.make_async_copy(dst, dst, recv).wait()

    def signal(sem, to_b, to_t):
        pl.semaphore_signal(sem, inc=1, device_id=(g, to_b, to_t), device_id_type=pl.DeviceIdType.MESH)

    own = [
        pltpu.make_async_copy(tok_hbm.at[of_wave(w), cols(b)], xs.at[w, b, t], local_sem.at[4])
        for w in range(WAVES)
    ]
    local = [
        pltpu.make_async_copy(tok_hbm, tok, local_sem.at[0]),
        pltpu.make_async_copy(wg_hbm, wg, local_sem.at[1]),
        pltpu.make_async_copy(wu_hbm, wu, local_sem.at[2]),
        pltpu.make_async_copy(wd_hbm, wd, local_sem.at[3]),
    ]
    notes = [
        pltpu.make_async_copy(ids_hbm, ids, local_sem.at[5]),
        pltpu.make_async_copy(values_hbm, values, local_sem.at[6]),
    ]
    barrier = pltpu.get_barrier_semaphore()
    signal(barrier, b, pair)
    signal(barrier, b, across)
    signal(barrier, blk(1), t)

    @pl.when(inner)
    def _():
        signal(barrier, blk(3), t)

    for copy in notes + local[:1] + own + local[1:]:
        copy.start()
    for copy in notes:
        copy.wait()
    meta[noted(b, t)] = jnp.zeros((SUBLANES, LANES), f32)
    meta[noted(b, t), 0:1, :all_rows] = ids[...].astype(f32)
    meta[noted(b, t), 1:2, :all_rows] = values[...]

    @pl.when(inner)
    def _():
        pl.semaphore_wait(barrier, 4)
        signal(far.at[0], blk(1), t)
        signal(far.at[0], blk(3), t)

    @pl.when(outer)
    def _():
        pl.semaphore_wait(barrier, 3)

    local[0].wait()
    arrived(fin_send.at[:, 0], local_sem.at[4])

    def far_known():
        pl.semaphore_wait(far.at[0], 1)

        @pl.when(inner)
        def _():
            signal(far.at[1], blk(1), t)

    def far_end():
        @pl.when(outer)
        def _():
            pl.semaphore_wait(far.at[1], 1)

    ready = {"weights": False, "down": False, "far": False, "end": False}

    def launch(w, k):
        if k == 2 and not ready["far"]:
            far_known()
            ready["far"] = True
        if k == 3 and not ready["end"]:
            far_end()
            ready["end"] = True
        if w == 0:
            note = meta.at[noted(b, t)]
            remote(note, note, 9, m_recv.at[0, k], blk(k), t)
        remote(tok.at[of_wave(w), cols(blk(k))], xs.at[w, b, t], 0, z_recv.at[w, k - 1], blk(k), t)

    def spread(w, k):
        source = blk(k)
        mine = xs.at[w, source, t]
        if w == 0:
            note = meta.at[noted(source, t)]
            if k:
                arrived(note, m_recv.at[0, k])
            remote(note, note, 9, m_recv.at[1, k], b, across)
            remote(note, note, 9, m_recv.at[2, k], b, pair)
        if k:
            arrived(mine, z_recv.at[w, k - 1])
        remote(mine, mine, 1, x_recv.at[w, k], b, across)
        remote(mine, mine, 2, c_recv.at[w, k], b, pair)

    def pass_on(w, k):
        source = blk(k)
        theirs = xs.at[w, source, across]
        if w == 0:
            note = meta.at[noted(source, across)]
            arrived(note, m_recv.at[1, k])
            remote(note, note, 9, m_recv.at[2, k], b, pair)
        arrived(theirs, x_recv.at[w, k])
        remote(theirs, theirs, 2, c_recv.at[w, k], b, pair)

    def wide(mask, size):
        return jnp.concatenate([mask] * (size // LANES), axis=1)

    def prepare(k):
        source = blk(k)
        arrived(meta.at[pl.ds(0, 2)], m_recv.at[2, k])
        turned = jnp.transpose(meta[pl.ds(source * nt, nt)].reshape(nt * SUBLANES, LANES))
        for row, out in ((0, routes),) if k else ((0, routes), (1, scales)):
            for w in range(WAVES):
                column = jnp.concatenate(
                    [turned[w * rows:(w + 1) * rows, SUBLANES * i + row:SUBLANES * i + row + 1] for i in range(nt)],
                    axis=0,
                )
                out[w, k] = jnp.broadcast_to(column, (block, LANES))

    def contract(w, k):
        source = blk(k)
        if w == 0:
            prepare(k)
        arrived(xs.at[w, source, pl.ds(0, 2)], c_recv.at[w, k])
        if not ready["weights"]:
            local[1].wait()
            local[2].wait()
            ready["weights"] = True
        chosen = wide(routes[w, k], ff)
        x = xs[w, source].reshape(block, width)
        for at, weights in ((0, wg), (ff, wu)):
            total = None
            for e in range(experts):
                value = jnp.dot(x, weights[e], preferred_element_type=f32)
                total = value if e == 0 else jnp.where(chosen == e, value, total)
            part[w, k, :, at:at + ff] = total
            if k:
                part_send[w, k, :, at:at + ff] = total.astype(bf16)
        if k == 1:
            remote(part_send.at[w, 1], part_recv.at[w, 0], 6, p_recv.at[w, 0], blk(1), t)
        elif k:
            @pl.when(outer)
            def _():
                remote(part_send.at[w, k], part_recv.at[w, 5 - k], 6, p_recv.at[w, 5 - k], blk(1), t)

    def relay(w, k):
        @pl.when(inner)
        def _():
            arrived(part_recv.at[w, k], p_recv.at[w, k])
            part_send[w, k] = (part[w, k] + part_recv[w, k].astype(f32)).astype(bf16)
            remote(part_send.at[w, k], part_recv.at[w, 1], 6, p_recv.at[w, 1], blk(k), t)

    def activate(w, k):
        total = part[w, 0]
        for slot in (0, 1):
            arrived(part_recv.at[w, slot], p_recv.at[w, slot])
            total = total + part_recv[w, slot].astype(f32)
        gate, up = total[:, :ff], total[:, ff:]
        hid[w, b] = (gate / (1.0 + jnp.exp(-gate)) * up * wide(scales[w, 0], ff)).astype(bf16)
        mine = hid.at[w, b]

        @pl.when(inner)
        def _():
            remote(mine, mine, 7, h_recv.at[w, 2], blk(3), t)

        remote(mine, mine, 7, h_recv.at[w, 0], blk(1), t)

        @pl.when(outer)
        def _():
            remote(mine, mine, 7, h_recv.at[w, 1], blk(2), t)

    def forward(w, k):
        @pl.when(inner)
        def _():
            source = blk(k)
            theirs = hid.at[w, source]
            arrived(theirs, h_recv.at[w, k - 1])
            if k == 1:
                remote(theirs, theirs, 8, h_recv.at[w, 1], blk(3), t)
            else:
                remote(theirs, theirs, 8, h_recv.at[w, 4 - k], blk(1), t)

    def expand(w, k):
        source = blk(k)
        if not ready["down"]:
            local[3].wait()
            ready["down"] = True
        if k:
            if k in (2, 3):
                @pl.when(outer)
                def _():
                    arrived(hid.at[w, source], h_recv.at[w, k - 1])
            else:
                arrived(hid.at[w, source], h_recv.at[w, k - 1])
        chosen = wide(routes[w, k], ff)
        h = hid[w, source].astype(f32)
        routed = jnp.concatenate([jnp.where(chosen == e, h, 0.0).astype(bf16) for e in range(experts)], axis=1)
        ys[w, k] = jnp.dot(routed, wd[...].reshape(experts * ff, width), preferred_element_type=f32)
        for j, place in ((1, across_pair), (0, pair)):
            remote(ys.at[w, k, owned(place)], ycore.at[w, k, j], 3, y_recv.at[w, k], b, pair)

    def exchange(w, k):
        arrived(ycore.at[w, k], y_recv.at[w, k])
        yx_send[w, k] = (ys[w, k, owned(across), :] + ycore[w, k, 1]).astype(bf16)
        remote(yx_send.at[w, k], yx_recv.at[w, k], 4, yx_sem.at[w, k], b, across)

    def finish(w, k):
        total = ys[w, k, owned(t), :] + ycore[w, k, 0]
        arrived(yx_recv.at[w, k], yx_sem.at[w, k])
        total = total + yx_recv[w, k].astype(f32)
        if k:
            fin_send[w, k] = total.astype(bf16)
            remote(fin_send.at[w, k], out_ref.at[of_wave(w), cols(b)], 5, o_recv.at[0], blk(k), t)
        else:
            out_ref[of_wave(w), cols(b)] = total.astype(bf16)

    steps = {
        "Z": launch, "S": spread, "P": pass_on, "C": contract, "R": relay,
        "A": activate, "H": forward, "E": expand, "X": exchange, "F": finish,
    }
    for name, w, k in ORDER:
        steps[name](w, k)

    others = fin_send.at[:, pl.ds(1, nb - 1)]
    arrived(others, o_recv.at[0])
    for kind, ref in (
        (0, others), (1, yx_send), (2, xs.at[:, :, pl.ds(0, 2)]), (3, ycore), (4, yx_send), (5, others),
        (6, part_send.at[:, pl.ds(1, nb - 1)]), (9, meta.at[pl.ds(0, nb * nt - 1)]),
    ):
        arrived(ref, send_sem.at[kind])

    @pl.when(inner)
    def _():
        arrived(hid.at[:, pl.ds(0, 2)], send_sem.at[7])
        arrived(hid.at[:, pl.ds(0, 2)], send_sem.at[8])

    @pl.when(outer)
    def _():
        arrived(hid.at[:, pl.ds(0, 2)], send_sem.at[7])


def stationary_body(nb, nt, tokens, expert_ids, gate_values, w_gate, w_up, w_down):
    rows, features = tokens.shape
    experts, width, ff = w_gate.shape
    f32, bf16 = jnp.float32, jnp.bfloat16
    wave_rows = rows // WAVES
    block = nt * wave_rows
    dma = pltpu.SemaphoreType.DMA
    vmem = pl.BlockSpec(memory_space=pltpu.VMEM)
    hbm = pl.BlockSpec(memory_space=pltpu.HBM)
    each = (WAVES, nb)
    return pl.pallas_call(
        functools.partial(kernel, nb, nt),
        out_shape=pltpu.VMEM((rows, features), bf16),
        in_specs=[hbm] * 6,
        out_specs=vmem,
        scratch_shapes=[
            pltpu.VMEM((rows, features), bf16),
            pltpu.VMEM((1, rows), jnp.int32),
            pltpu.VMEM((1, rows), f32),
            pltpu.VMEM((nb * nt, SUBLANES, LANES), f32),
            pltpu.VMEM(w_gate.shape, bf16),
            pltpu.VMEM(w_up.shape, bf16),
            pltpu.VMEM(w_down.shape, bf16),
            pltpu.VMEM((*each, block, LANES), f32),
            pltpu.VMEM((WAVES, 1, block, LANES), f32),
            pltpu.VMEM((*each, nt, wave_rows, width), bf16),
            pltpu.VMEM((*each, block, 2 * ff), f32),
            pltpu.VMEM((*each, block, 2 * ff), bf16),
            pltpu.VMEM((*each, block, 2 * ff), bf16),
            pltpu.VMEM((*each, block, ff), bf16),
            pltpu.VMEM((*each, block, width), f32),
            pltpu.VMEM((*each, 2, wave_rows, width), f32),
            pltpu.VMEM((*each, wave_rows, width), bf16),
            pltpu.VMEM((*each, wave_rows, width), bf16),
            pltpu.VMEM((*each, wave_rows, width), bf16),
            dma((7,)),
            dma((10,)),
            pltpu.SemaphoreType.REGULAR((2,)),
            dma((3, nb)),
            dma((WAVES, nb - 1)), dma(each), dma(each), dma(each), dma((WAVES, nb - 1)), dma(each), dma(each), dma((1,)),
        ],
        compiler_params=pltpu.CompilerParams(
            collective_id=0, has_side_effects=True, vmem_limit_bytes=60000000,
        ),
    )(tokens, expert_ids.reshape(1, rows), gate_values.reshape(1, rows), w_gate, w_up, w_down)


def solution(mesh):
    nb, nt = mesh.shape["blk"], mesh.shape["tok"]

    def body(tokens, expert_ids, gate_values, w_gate, w_up, w_down):
        rows = tokens.shape[0]
        width, ff = w_gate.shape[1], w_gate.shape[2]
        fits = width % LANES == 0 and ff % LANES == 0 and rows % (16 * WAVES) == 0 and rows <= LANES
        if fits and nt == 4 and nb == 4:
            return stationary_body(nb, nt, tokens, expert_ids, gate_values, w_gate, w_up, w_down)
        return gathered_body(tokens, expert_ids, gate_values, w_gate, w_up, w_down)

    return jax.shard_map(
        body,
        mesh=mesh,
        in_specs=(
            P(("groups", "blk", "tok"), None),
            P(("groups", "blk", "tok"), None),
            P(("groups", "blk", "tok"), None),
            P(None, "blk", "tok"),
            P(None, "blk", "tok"),
            P(None, "tok", "blk"),
        ),
        out_specs=P(("groups", "blk", "tok"), None),
        check_vma=False,
    )
```

```python
import functools

import jax
import jax.numpy as jnp
from jax import lax
from jax.experimental import pallas as pl
from jax.experimental.pallas import tpu as pltpu
from jax.sharding import PartitionSpec as P

LANES = 128
SUBLANES = 8
WAVES = 4
OUTER_ORDER = (
    ("S", 0, 0), ("Z", 0, 1), ("Z", 2, 1), ("S", 1, 0), ("Z", 1, 1), ("S", 2, 0), ("Z", 3, 1),
    ("S", 3, 0), ("Z", 1, 2), ("Z", 2, 2), ("P", 0, 0), ("Z", 1, 3), ("S", 0, 1), ("Z", 0, 3),
    ("Z", 3, 3), ("Z", 2, 3), ("P", 1, 0), ("C", 0, 0), ("P", 2, 0), ("Z", 0, 2), ("C", 1, 0),
    ("P", 3, 0), ("S", 1, 2), ("C", 2, 0), ("S", 3, 2), ("P", 0, 1), ("C", 3, 0), ("Z", 3, 2),
    ("C", 0, 1), ("P", 1, 2), ("S", 1, 3), ("S", 0, 3), ("P", 3, 2), ("C", 1, 2), ("S", 0, 2),
    ("S", 3, 3), ("C", 3, 2), ("S", 2, 3), ("P", 1, 3), ("P", 0, 3), ("C", 1, 3), ("S", 1, 1),
    ("P", 0, 2), ("C", 0, 3), ("C", 0, 2), ("P", 3, 3), ("P", 2, 3), ("C", 3, 3), ("C", 2, 3),
    ("P", 1, 1), ("S", 3, 1), ("C", 1, 1), ("S", 2, 2), ("S", 2, 1), ("P", 3, 1), ("P", 2, 2),
    ("C", 3, 1), ("A", 1, 0), ("C", 2, 2), ("P", 2, 1), ("E", 1, 0), ("A", 0, 0), ("E", 0, 0),
    ("C", 2, 1), ("X", 1, 0), ("X", 0, 0), ("A", 3, 0), ("E", 3, 0), ("E", 0, 1), ("F", 0, 0),
    ("X", 3, 0), ("A", 2, 0), ("E", 2, 0), ("E", 1, 1), ("X", 0, 1), ("E", 3, 1), ("X", 2, 0),
    ("X", 1, 1), ("X", 3, 1), ("F", 3, 0), ("E", 0, 2), ("E", 1, 2), ("F", 0, 1), ("X", 0, 2),
    ("F", 2, 0), ("E", 3, 2), ("F", 1, 1), ("X", 1, 2), ("E", 1, 3), ("F", 3, 1), ("X", 3, 2),
    ("F", 1, 0), ("X", 1, 3), ("E", 2, 1), ("F", 0, 2), ("E", 0, 3), ("X", 2, 1), ("F", 1, 2),
    ("E", 3, 3), ("X", 0, 3), ("F", 3, 2), ("E", 2, 3), ("F", 1, 3), ("X", 3, 3), ("E", 2, 2),
    ("X", 2, 3), ("F", 2, 1), ("X", 2, 2), ("F", 0, 3), ("F", 3, 3), ("F", 2, 3), ("F", 2, 2),
)
INNER_ORDER = (
    ("Z", 1, 3), ("Z", 3, 3), ("S", 2, 0), ("S", 1, 0), ("Z", 0, 1), ("S", 3, 0), ("S", 0, 0),
    ("Z", 1, 2), ("Z", 3, 2), ("S", 1, 3), ("S", 0, 1), ("P", 2, 0), ("S", 3, 3), ("S", 2, 1),
    ("P", 1, 0), ("C", 2, 0), ("S", 1, 1), ("P", 3, 0), ("C", 1, 0), ("P", 0, 0), ("S", 3, 1),
    ("Z", 0, 2), ("C", 3, 0), ("P", 1, 3), ("S", 1, 2), ("C", 0, 0), ("P", 0, 1), ("S", 2, 2),
    ("C", 1, 3), ("P", 3, 3), ("C", 0, 1), ("Z", 1, 1), ("P", 2, 1), ("P", 1, 1), ("C", 3, 3),
    ("Z", 0, 3), ("P", 3, 1), ("C", 2, 1), ("C", 1, 1), ("Z", 3, 1), ("C", 3, 1), ("Z", 2, 3),
    ("S", 0, 2), ("P", 1, 2), ("P", 2, 2), ("S", 3, 2), ("C", 1, 2), ("C", 2, 2), ("S", 0, 3),
    ("Z", 2, 2), ("R", 1, 3), ("S", 2, 3), ("P", 0, 2), ("P", 3, 2), ("C", 0, 2), ("Z", 2, 1),
    ("R", 3, 3), ("C", 3, 2), ("P", 0, 3), ("R", 1, 2), ("P", 2, 3), ("C", 0, 3), ("C", 2, 3),
    ("R", 0, 2), ("R", 0, 3), ("R", 3, 2), ("R", 2, 2), ("A", 0, 0), ("E", 0, 0), ("A", 1, 0),
    ("E", 1, 0), ("X", 0, 0), ("A", 3, 0), ("E", 3, 0), ("X", 1, 0), ("H", 1, 1), ("E", 1, 1),
    ("X", 3, 0), ("X", 1, 1), ("R", 2, 3), ("H", 0, 3), ("E", 0, 3), ("H", 0, 1), ("E", 0, 1),
    ("H", 1, 3), ("E", 1, 3), ("F", 1, 0), ("X", 0, 3), ("H", 3, 3), ("E", 3, 3), ("X", 0, 1),
    ("F", 3, 0), ("H", 1, 2), ("E", 1, 2), ("X", 1, 3), ("H", 3, 1), ("E", 3, 1), ("X", 3, 3),
    ("F", 1, 1), ("H", 2, 1), ("E", 2, 1), ("X", 1, 2), ("A", 2, 0), ("E", 2, 0), ("X", 3, 1),
    ("H", 0, 2), ("F", 0, 3), ("E", 0, 2), ("X", 2, 1), ("F", 0, 1), ("X", 2, 0), ("F", 1, 3),
    ("H", 3, 2), ("E", 3, 2), ("X", 0, 2), ("F", 3, 3), ("H", 2, 2), ("E", 2, 2), ("X", 3, 2),
    ("F", 0, 0), ("H", 2, 3), ("E", 2, 3), ("F", 3, 1), ("X", 2, 2), ("F", 1, 2), ("F", 2, 1),
    ("X", 2, 3), ("F", 2, 0), ("F", 0, 2), ("F", 3, 2), ("F", 2, 2), ("F", 2, 3),
)


def gathered_body(tokens, expert_ids, gate_values, w_gate, w_up, w_down):
    group_rows = lax.all_gather(tokens, "tok", axis=0, tiled=True)
    group_routes = lax.all_gather(expert_ids, "tok", axis=0, tiled=True)[:, 0]
    experts = w_gate.shape[0]
    count_rows = group_rows.shape[0]
    capacity = 3 * count_rows // 4
    expert_range = jnp.arange(experts, dtype=jnp.int32)
    onehot = (group_routes[:, None] == expert_range[None, :]).astype(jnp.int32)
    slot_rank = jnp.sum((jnp.cumsum(onehot, axis=0) - onehot) * onehot, axis=1)
    expert_match = group_routes[None, None, :] == expert_range[:, None, None]
    slot_match = slot_rank[None, None, :] == jnp.arange(capacity, dtype=jnp.int32)[None, :, None]
    dispatch = (expert_match & slot_match).astype(jnp.bfloat16)
    slots = jnp.einsum(
        "esg,gd->esd", dispatch, group_rows, preferred_element_type=jnp.float32
    ).astype(jnp.bfloat16)

    def add_part(weights):
        return jnp.einsum("esd,edf->esf", slots, weights, preferred_element_type=jnp.float32)

    gate_sum = add_part(lax.all_gather(w_gate, "blk", axis=1, tiled=True))
    up_sum = add_part(lax.all_gather(w_up, "blk", axis=1, tiled=True))
    hidden = (jax.nn.silu(gate_sum) * up_sum).astype(jnp.bfloat16)
    slot_out = jnp.einsum(
        "esf,efd->esd",
        hidden,
        lax.all_gather(w_down, "blk", axis=2, tiled=True),
        preferred_element_type=jnp.float32,
    )
    flat_rows = slot_out.reshape(experts * capacity, slot_out.shape[2])
    position = group_routes * capacity + slot_rank
    partial_value = jnp.take(flat_rows, position, axis=0)
    summed = lax.psum_scatter(partial_value, "tok", scatter_dimension=0, tiled=True)
    return (gate_values * summed).astype(jnp.bfloat16)


def kernel(
    nb, nt, tok_hbm, ids_hbm, values_hbm, wg_hbm, wu_hbm, wd_hbm, out_ref,
    tok, ids, values, meta, wg, wu, wd, routes, scales, xs, part, part_send, part_recv, hid, ys, ycore,
    yx_send, yx_recv, fin_send,
    local_sem, send_sem, far, m_recv, z_recv, x_recv, c_recv, p_recv, h_recv, y_recv, yx_sem, o_recv,
):
    g, b, t = lax.axis_index("groups"), lax.axis_index("blk"), lax.axis_index("tok")
    all_rows, width = tok.shape[0], xs.shape[4]
    rows = all_rows // WAVES
    block = nt * rows
    experts, ff = wg.shape[0], wg.shape[2]
    f32, bf16 = jnp.float32, jnp.bfloat16
    pair = t + 1 - 2 * lax.rem(t, 2)
    across = lax.rem(t + 2, nt)
    across_pair = lax.rem(pair + 2, nt)
    outer = lax.rem((b + 1) // 2 + 1, 2) == 1
    inner = jnp.logical_not(outer)

    low, high = lax.rem(b, 2), b // 2
    blocks = [b, 2 * high + 1 - low, 2 * (1 - high) + low, 2 * (1 - high) + 1 - low]

    def blk(k):
        return blocks[k]

    def cols(index):
        return pl.ds(pl.multiple_of(index * width, LANES), width)

    def of_wave(w):
        return pl.ds(w * rows, rows)

    def noted(block_at, token_at):
        return block_at * nt + token_at

    def owned(index):
        return pl.ds(pl.multiple_of(index * rows, SUBLANES), rows)

    def remote(src, dst, kind, recv, to_b, to_t):
        pltpu.make_async_remote_copy(
            src_ref=src, dst_ref=dst, send_sem=send_sem.at[kind], recv_sem=recv,
            device_id=(g, to_b, to_t), device_id_type=pl.DeviceIdType.MESH,
        ).start()

    def arrived(dst, recv):
        pltpu.make_async_copy(dst, dst, recv).wait()

    def signal(sem, to_b, to_t):
        pl.semaphore_signal(sem, inc=1, device_id=(g, to_b, to_t), device_id_type=pl.DeviceIdType.MESH)

    own = [
        pltpu.make_async_copy(tok_hbm.at[of_wave(w), cols(b)], xs.at[w, b, t], local_sem.at[4])
        for w in range(WAVES)
    ]
    local = [
        pltpu.make_async_copy(tok_hbm, tok, local_sem.at[0]),
        pltpu.make_async_copy(wg_hbm, wg, local_sem.at[1]),
        pltpu.make_async_copy(wu_hbm, wu, local_sem.at[2]),
        pltpu.make_async_copy(wd_hbm, wd, local_sem.at[3]),
    ]
    notes = [
        pltpu.make_async_copy(ids_hbm, ids, local_sem.at[5]),
        pltpu.make_async_copy(values_hbm, values, local_sem.at[6]),
    ]
    barrier = pltpu.get_barrier_semaphore()
    signal(barrier, b, pair)
    signal(barrier, b, across)
    signal(barrier, blk(1), t)

    @pl.when(inner)
    def _():
        signal(barrier, blk(3), t)

    for copy in notes + local[:1] + own + local[1:]:
        copy.start()
    for copy in notes:
        copy.wait()
    meta[noted(b, t)] = jnp.zeros((SUBLANES, LANES), f32)
    meta[noted(b, t), 0:1, :all_rows] = ids[...].astype(f32)
    meta[noted(b, t), 1:2, :all_rows] = values[...]

    @pl.when(inner)
    def _():
        pl.semaphore_wait(barrier, 4)
        signal(far.at[0], blk(1), t)
        signal(far.at[0], blk(3), t)

    @pl.when(outer)
    def _():
        pl.semaphore_wait(barrier, 3)

    local[0].wait()
    arrived(fin_send.at[:, 0], local_sem.at[4])

    ready = set()

    def once(*name):
        if name in ready:
            return False
        ready.add(name)
        return True

    def only(side):
        def call(step):
            if side in ready:
                step()
        return call

    def announced(k):
        if k == 2 and once("far"):
            pl.semaphore_wait(far.at[0], 1)
            if "inner" in ready:
                signal(far.at[1], blk(1), t)
        if k == 3 and "outer" in ready and once("end"):
            pl.semaphore_wait(far.at[1], 1)

    def launch(w, k):
        announced(k)
        if once("launch", k):
            note = meta.at[noted(b, t)]
            remote(note, note, 9, m_recv.at[0, k], blk(k), t)
        remote(tok.at[of_wave(w), cols(blk(k))], xs.at[w, b, t], 0, z_recv.at[w, k - 1], blk(k), t)

    def spread(w, k):
        source = blk(k)
        mine = xs.at[w, source, t]
        if once("spread", k):
            note = meta.at[noted(source, t)]
            if k:
                arrived(note, m_recv.at[0, k])
            remote(note, note, 9, m_recv.at[1, k], b, across)
            remote(note, note, 9, m_recv.at[2, k], b, pair)
        if k:
            arrived(mine, z_recv.at[w, k - 1])
        remote(mine, mine, 1, x_recv.at[w, k], b, across)
        remote(mine, mine, 2, c_recv.at[w, k], b, pair)

    def pass_on(w, k):
        source = blk(k)
        theirs = xs.at[w, source, across]
        if once("pass", k):
            note = meta.at[noted(source, across)]
            arrived(note, m_recv.at[1, k])
            remote(note, note, 9, m_recv.at[2, k], b, pair)
        arrived(theirs, x_recv.at[w, k])
        remote(theirs, theirs, 2, c_recv.at[w, k], b, pair)

    def wide(mask, size):
        return jnp.concatenate([mask] * (size // LANES), axis=1)

    def prepare(k):
        source = blk(k)
        arrived(meta.at[pl.ds(0, 2)], m_recv.at[2, k])
        turned = jnp.transpose(meta[pl.ds(source * nt, nt)].reshape(nt * SUBLANES, LANES))
        for row, out in ((0, routes),) if k else ((0, routes), (1, scales)):
            for w in range(WAVES):
                column = jnp.concatenate(
                    [turned[w * rows:(w + 1) * rows, SUBLANES * i + row:SUBLANES * i + row + 1] for i in range(nt)],
                    axis=0,
                )
                out[w, k] = jnp.broadcast_to(column, (block, LANES))

    def contract(w, k):
        source = blk(k)
        if once("note", k):
            prepare(k)
        arrived(xs.at[w, source, pl.ds(0, 2)], c_recv.at[w, k])
        if once("up"):
            local[1].wait()
            local[2].wait()
        chosen = wide(routes[w, k], ff)
        x = xs[w, source].reshape(block, width)
        for at, weights in ((0, wg), (ff, wu)):
            total = None
            for e in range(experts):
                value = jnp.dot(x, weights[e], preferred_element_type=f32)
                total = value if e == 0 else jnp.where(chosen == e, value, total)
            part[w, k, :, at:at + ff] = total
            if k:
                part_send[w, k, :, at:at + ff] = total.astype(bf16)
        if k == 1:
            remote(part_send.at[w, 1], part_recv.at[w, 0], 6, p_recv.at[w, 0], blk(1), t)
        elif k:
            @only("outer")
            def _():
                remote(part_send.at[w, k], part_recv.at[w, 5 - k], 6, p_recv.at[w, 5 - k], blk(1), t)

    def relay(w, k):
        @only("inner")
        def _():
            arrived(part_recv.at[w, k], p_recv.at[w, k])
            part_send[w, k] = (part[w, k] + part_recv[w, k].astype(f32)).astype(bf16)
            remote(part_send.at[w, k], part_recv.at[w, 1], 6, p_recv.at[w, 1], blk(k), t)

    def activate(w, k):
        total = part[w, 0]
        for slot in (0, 1):
            arrived(part_recv.at[w, slot], p_recv.at[w, slot])
            total = total + part_recv[w, slot].astype(f32)
        gate, up = total[:, :ff], total[:, ff:]
        hid[w, b] = (gate / (1.0 + jnp.exp(-gate)) * up * wide(scales[w, 0], ff)).astype(bf16)
        mine = hid.at[w, b]

        @only("inner")
        def _():
            remote(mine, mine, 7, h_recv.at[w, 2], blk(3), t)

        remote(mine, mine, 7, h_recv.at[w, 0], blk(1), t)

    def forward(w, k):
        @only("inner")
        def _():
            source = blk(k)
            theirs = hid.at[w, source]
            arrived(theirs, h_recv.at[w, k - 1])
            if k == 1:
                remote(theirs, theirs, 8, h_recv.at[w, 1], blk(3), t)
            else:
                remote(theirs, theirs, 8, h_recv.at[w, 4 - k], blk(1), t)

    def expand(w, k):
        source = blk(k)
        if once("down"):
            local[3].wait()
        if k:
            if k in (1, 2, 3):
                @only("outer")
                def _():
                    arrived(hid.at[w, source], h_recv.at[w, k - 1])
            else:
                arrived(hid.at[w, source], h_recv.at[w, k - 1])
        chosen = wide(routes[w, k], ff)
        h = hid[w, source].astype(f32)
        routed = jnp.concatenate([jnp.where(chosen == e, h, 0.0).astype(bf16) for e in range(experts)], axis=1)
        ys[w, k] = jnp.dot(routed, wd[...].reshape(experts * ff, width), preferred_element_type=f32)
        for j, place in ((1, across_pair), (0, pair)):
            remote(ys.at[w, k, owned(place)], ycore.at[w, k, j], 3, y_recv.at[w, k], b, pair)

    def exchange(w, k):
        arrived(ycore.at[w, k], y_recv.at[w, k])
        yx_send[w, k] = (ys[w, k, owned(across), :] + ycore[w, k, 1]).astype(bf16)
        remote(yx_send.at[w, k], yx_recv.at[w, k], 4, yx_sem.at[w, k], b, across)

    def finish(w, k):
        total = ys[w, k, owned(t), :] + ycore[w, k, 0]
        arrived(yx_recv.at[w, k], yx_sem.at[w, k])
        total = total + yx_recv[w, k].astype(f32)
        if k:
            fin_send[w, k] = total.astype(bf16)
            remote(fin_send.at[w, k], out_ref.at[of_wave(w), cols(b)], 5, o_recv.at[0], blk(k), t)
        else:
            out_ref[of_wave(w), cols(b)] = total.astype(bf16)

    steps = {
        "Z": launch, "S": spread, "P": pass_on, "C": contract, "R": relay,
        "A": activate, "H": forward, "E": expand, "X": exchange, "F": finish,
    }
    def run(side, order):
        ready.clear()
        ready.add(side)
        for name, w, k in order:
            if side == "inner" and name != "Z" and (name, k) != ("S", 0):
                announced(2)
            steps[name](w, k)
        others = fin_send.at[:, pl.ds(1, nb - 1)]
        arrived(others, o_recv.at[0])
        for kind, ref in (
            (0, others), (1, yx_send), (2, xs.at[:, :, pl.ds(0, 2)]), (3, ycore), (4, yx_send), (5, others),
            (6, part_send.at[:, pl.ds(1, nb - 1)]), (9, meta.at[pl.ds(0, nb * nt - 1)]),
        ):
            arrived(ref, send_sem.at[kind])

        @only("inner")
        def _():
            arrived(hid.at[:, pl.ds(0, 2)], send_sem.at[7])
            arrived(hid.at[:, pl.ds(0, 3)], send_sem.at[8])

        @only("outer")
        def _():
            arrived(hid.at[:, pl.ds(0, 1)], send_sem.at[7])

    @pl.when(inner)
    def _():
        run("inner", INNER_ORDER)

    @pl.when(outer)
    def _():
        run("outer", OUTER_ORDER)


def stationary_body(nb, nt, tokens, expert_ids, gate_values, w_gate, w_up, w_down):
    rows, features = tokens.shape
    experts, width, ff = w_gate.shape
    f32, bf16 = jnp.float32, jnp.bfloat16
    wave_rows = rows // WAVES
    block = nt * wave_rows
    dma = pltpu.SemaphoreType.DMA
    hbm = pl.BlockSpec(memory_space=pltpu.HBM)
    each = (WAVES, nb)
    return pl.pallas_call(
        functools.partial(kernel, nb, nt),
        out_shape=pltpu.VMEM((rows, features), bf16),
        in_specs=[hbm] * 6,
        out_specs=pl.BlockSpec(memory_space=pltpu.VMEM),
        scratch_shapes=[
            pltpu.VMEM((rows, features), bf16),
            pltpu.VMEM((1, rows), jnp.int32),
            pltpu.VMEM((1, rows), f32),
            pltpu.VMEM((nb * nt, SUBLANES, LANES), f32),
            pltpu.VMEM(w_gate.shape, bf16),
            pltpu.VMEM(w_up.shape, bf16),
            pltpu.VMEM(w_down.shape, bf16),
            pltpu.VMEM((*each, block, LANES), f32),
            pltpu.VMEM((WAVES, 1, block, LANES), f32),
            pltpu.VMEM((*each, nt, wave_rows, width), bf16),
            pltpu.VMEM((*each, block, 2 * ff), f32),
            pltpu.VMEM((*each, block, 2 * ff), bf16),
            pltpu.VMEM((*each, block, 2 * ff), bf16),
            pltpu.VMEM((*each, block, ff), bf16),
            pltpu.VMEM((*each, block, width), f32),
            pltpu.VMEM((*each, 2, wave_rows, width), f32),
            pltpu.VMEM((*each, wave_rows, width), bf16),
            pltpu.VMEM((*each, wave_rows, width), bf16),
            pltpu.VMEM((*each, wave_rows, width), bf16),
            dma((7,)),
            dma((10,)),
            pltpu.SemaphoreType.REGULAR((2,)),
            dma((3, nb)),
            dma((WAVES, nb - 1)), dma(each), dma(each), dma(each), dma((WAVES, nb - 1)), dma(each), dma(each), dma((1,)),
        ],
        compiler_params=pltpu.CompilerParams(
            collective_id=0, has_side_effects=True, vmem_limit_bytes=60_000_000,
        ),
    )(tokens, expert_ids.reshape(1, rows), gate_values.reshape(1, rows), w_gate, w_up, w_down)


def solution(mesh):
    nb, nt = mesh.shape["blk"], mesh.shape["tok"]

    def body(tokens, expert_ids, gate_values, w_gate, w_up, w_down):
        rows = tokens.shape[0]
        width, ff = w_gate.shape[1], w_gate.shape[2]
        fits = width % LANES == 0 and ff % LANES == 0 and rows % (16 * WAVES) == 0 and rows <= LANES
        if fits and nt == 4 and nb == 4:
            return stationary_body(nb, nt, tokens, expert_ids, gate_values, w_gate, w_up, w_down)
        return gathered_body(tokens, expert_ids, gate_values, w_gate, w_up, w_down)

    return jax.shard_map(
        body,
        mesh=mesh,
        in_specs=(
            P(("groups", "blk", "tok"), None),
            P(("groups", "blk", "tok"), None),
            P(("groups", "blk", "tok"), None),
            P(None, "blk", "tok"),
            P(None, "blk", "tok"),
            P(None, "tok", "blk"),
        ),
        out_specs=P(("groups", "blk", "tok"), None),
        check_vma=False,
    )
```

```python
import functools

import jax
import jax.numpy as jnp
from jax import lax
from jax.experimental import pallas as pl
from jax.experimental.pallas import tpu as pltpu
from jax.sharding import PartitionSpec as P

LANES = 128
SUBLANES = 8
WAVES = 4
OUTER_ORDER = (
    ("S", 2, 0), ("Z", 2, 1), ("S", 3, 0), ("Z", 0, 1), ("Z", 3, 1), ("S", 1, 0), ("S", 0, 0),
    ("Z", 2, 2), ("Z", 1, 3), ("Z", 2, 3), ("Z", 3, 3), ("Z", 0, 3), ("S", 3, 1), ("P", 2, 0),
    ("P", 3, 0), ("C", 2, 0), ("P", 1, 0), ("C", 3, 0), ("P", 0, 0), ("S", 0, 2), ("Z", 1, 1),
    ("C", 1, 0), ("C", 0, 0), ("Z", 1, 2), ("P", 3, 1), ("S", 2, 2), ("Z", 3, 2), ("C", 3, 1),
    ("S", 1, 3), ("Z", 0, 2), ("S", 2, 3), ("P", 0, 2), ("S", 3, 3), ("C", 0, 2), ("P", 2, 2),
    ("S", 0, 3), ("S", 3, 2), ("C", 2, 2), ("P", 1, 3), ("S", 2, 1), ("P", 2, 3), ("C", 1, 3),
    ("P", 3, 3), ("C", 2, 3), ("S", 0, 1), ("P", 0, 3), ("C", 3, 3), ("P", 3, 2), ("C", 0, 3),
    ("P", 2, 1), ("C", 3, 2), ("C", 2, 1), ("P", 0, 1), ("S", 1, 2), ("C", 0, 1), ("S", 1, 1),
    ("P", 1, 2), ("A", 1, 0), ("E", 1, 0), ("P", 1, 1), ("C", 1, 2), ("A", 2, 0), ("E", 2, 0),
    ("C", 1, 1), ("X", 1, 0), ("A", 3, 0), ("E", 3, 0), ("X", 2, 0), ("A", 0, 0), ("E", 0, 0),
    ("X", 3, 0), ("E", 2, 1), ("X", 0, 0), ("F", 2, 0), ("X", 2, 1), ("E", 0, 1), ("X", 0, 1),
    ("E", 3, 1), ("E", 2, 2), ("F", 0, 0), ("X", 3, 1), ("F", 3, 0), ("F", 2, 1), ("E", 0, 2),
    ("X", 2, 2), ("E", 1, 3), ("F", 0, 1), ("X", 0, 2), ("E", 3, 2), ("X", 1, 3), ("F", 3, 1),
    ("X", 3, 2), ("E", 1, 1), ("E", 2, 3), ("F", 2, 2), ("X", 1, 1), ("E", 3, 3), ("F", 0, 2),
    ("X", 2, 3), ("F", 1, 3), ("E", 0, 3), ("X", 3, 3), ("F", 1, 0), ("F", 3, 2), ("E", 1, 2),
    ("X", 0, 3), ("F", 1, 1), ("X", 1, 2), ("F", 2, 3), ("F", 3, 3), ("F", 0, 3), ("F", 1, 2),
)
INNER_ORDER = (
    ("Z", 3, 1), ("S", 2, 0), ("Z", 2, 3), ("Z", 0, 3), ("S", 1, 0), ("S", 0, 0), ("S", 3, 0),
    ("Z", 0, 2), ("Z", 2, 2), ("P", 2, 0), ("S", 2, 3), ("S", 2, 1), ("S", 0, 1), ("P", 1, 0),
    ("S", 0, 3), ("C", 2, 0), ("Z", 1, 3), ("S", 3, 1), ("Z", 3, 3), ("P", 0, 0), ("C", 1, 0),
    ("P", 3, 0), ("C", 0, 0), ("Z", 3, 2), ("C", 3, 0), ("S", 2, 2), ("P", 2, 3), ("P", 2, 1),
    ("C", 2, 3), ("P", 0, 1), ("Z", 2, 1), ("C", 2, 1), ("S", 1, 3), ("Z", 0, 1), ("P", 0, 3),
    ("P", 3, 1), ("S", 1, 1), ("C", 0, 1), ("S", 3, 3), ("C", 0, 3), ("C", 3, 1), ("P", 2, 2),
    ("S", 1, 2), ("C", 2, 2), ("S", 3, 2), ("P", 1, 3), ("P", 1, 1), ("C", 1, 3), ("P", 3, 3),
    ("Z", 1, 2), ("C", 1, 1), ("S", 0, 2), ("R", 0, 3), ("C", 3, 3), ("P", 1, 2), ("Z", 1, 1),
    ("P", 3, 2), ("R", 2, 3), ("C", 1, 2), ("C", 3, 2), ("R", 1, 2), ("P", 0, 2), ("R", 2, 2),
    ("C", 0, 2), ("R", 3, 2), ("R", 0, 2), ("R", 3, 3), ("A", 2, 0), ("E", 2, 0), ("A", 0, 0),
    ("X", 2, 0), ("E", 0, 0), ("H", 1, 1), ("E", 1, 1), ("X", 0, 0), ("A", 3, 0), ("E", 3, 0),
    ("X", 1, 1), ("R", 1, 3), ("H", 2, 3), ("E", 2, 3), ("H", 2, 1), ("E", 2, 1), ("X", 3, 0),
    ("X", 2, 3), ("H", 0, 3), ("E", 0, 3), ("X", 2, 1), ("H", 1, 2), ("E", 1, 2), ("H", 3, 1),
    ("E", 3, 1), ("X", 0, 3), ("H", 3, 3), ("E", 3, 3), ("H", 0, 1), ("E", 0, 1), ("X", 1, 2),
    ("F", 1, 1), ("X", 3, 1), ("X", 3, 3), ("A", 1, 0), ("E", 1, 0), ("F", 0, 0), ("X", 0, 1),
    ("F", 3, 0), ("F", 2, 3), ("H", 2, 2), ("E", 2, 2), ("X", 1, 0), ("H", 3, 2), ("E", 3, 2),
    ("F", 2, 0), ("F", 0, 3), ("X", 2, 2), ("H", 0, 2), ("E", 0, 2), ("F", 1, 2), ("X", 3, 2),
    ("H", 1, 3), ("E", 1, 3), ("F", 2, 1), ("F", 3, 3), ("X", 0, 2), ("F", 0, 1), ("X", 1, 3),
    ("F", 3, 1), ("F", 1, 0), ("F", 2, 2), ("F", 3, 2), ("F", 0, 2), ("F", 1, 3),
)


def gathered_body(tokens, expert_ids, gate_values, w_gate, w_up, w_down):
    group_rows = lax.all_gather(tokens, "tok", axis=0, tiled=True)
    group_routes = lax.all_gather(expert_ids, "tok", axis=0, tiled=True)[:, 0]
    experts = w_gate.shape[0]
    count_rows = group_rows.shape[0]
    capacity = 3 * count_rows // 4
    expert_range = jnp.arange(experts, dtype=jnp.int32)
    onehot = (group_routes[:, None] == expert_range[None, :]).astype(jnp.int32)
    slot_rank = jnp.sum((jnp.cumsum(onehot, axis=0) - onehot) * onehot, axis=1)
    expert_match = group_routes[None, None, :] == expert_range[:, None, None]
    slot_match = slot_rank[None, None, :] == jnp.arange(capacity, dtype=jnp.int32)[None, :, None]
    dispatch = (expert_match & slot_match).astype(jnp.bfloat16)
    slots = jnp.einsum(
        "esg,gd->esd", dispatch, group_rows, preferred_element_type=jnp.float32
    ).astype(jnp.bfloat16)

    def add_part(weights):
        return jnp.einsum("esd,edf->esf", slots, weights, preferred_element_type=jnp.float32)

    gate_sum = add_part(lax.all_gather(w_gate, "blk", axis=1, tiled=True))
    up_sum = add_part(lax.all_gather(w_up, "blk", axis=1, tiled=True))
    hidden = (jax.nn.silu(gate_sum) * up_sum).astype(jnp.bfloat16)
    slot_out = jnp.einsum(
        "esf,efd->esd",
        hidden,
        lax.all_gather(w_down, "blk", axis=2, tiled=True),
        preferred_element_type=jnp.float32,
    )
    flat_rows = slot_out.reshape(experts * capacity, slot_out.shape[2])
    position = group_routes * capacity + slot_rank
    partial_value = jnp.take(flat_rows, position, axis=0)
    summed = lax.psum_scatter(partial_value, "tok", scatter_dimension=0, tiled=True)
    return (gate_values * summed).astype(jnp.bfloat16)


def kernel(
    nb, nt, tok_hbm, ids_hbm, values_hbm, wg_hbm, wu_hbm, wd_hbm, out_ref,
    tok, ids, values, meta, wg, wu, wd, routes, scales, xs, part, part_send, part_recv, hid, ys, ycore,
    yx_send, yx_recv, fin_send,
    local_sem, send_sem, far, m_recv, z_recv, x_recv, c_recv, p_recv, h_recv, y_recv, yx_sem, o_recv,
):
    g, b, t = lax.axis_index("groups"), lax.axis_index("blk"), lax.axis_index("tok")
    all_rows, width = tok.shape[0], xs.shape[4]
    rows = all_rows // WAVES
    block = nt * rows
    experts, ff = wg.shape[0], wg.shape[2]
    f32, bf16 = jnp.float32, jnp.bfloat16
    pair = t + 1 - 2 * lax.rem(t, 2)
    across = lax.rem(t + 2, nt)
    across_pair = lax.rem(pair + 2, nt)
    outer = lax.rem((b + 1) // 2 + 1, 2) == 1
    inner = jnp.logical_not(outer)

    low, high = lax.rem(b, 2), b // 2
    blocks = [b, 2 * high + 1 - low, 2 * (1 - high) + low, 2 * (1 - high) + 1 - low]

    def blk(k):
        return blocks[k]

    def cols(index):
        return pl.ds(pl.multiple_of(index * width, LANES), width)

    def of_wave(w):
        return pl.ds(w * rows, rows)

    def noted(block_at, token_at):
        return block_at * nt + token_at

    def owned(index):
        return pl.ds(pl.multiple_of(index * rows, SUBLANES), rows)

    def remote(src, dst, kind, recv, to_b, to_t):
        pltpu.make_async_remote_copy(
            src_ref=src, dst_ref=dst, send_sem=send_sem.at[kind], recv_sem=recv,
            device_id=(g, to_b, to_t), device_id_type=pl.DeviceIdType.MESH,
        ).start()

    def arrived(dst, recv):
        pltpu.make_async_copy(dst, dst, recv).wait()

    def signal(sem, to_b, to_t):
        pl.semaphore_signal(sem, inc=1, device_id=(g, to_b, to_t), device_id_type=pl.DeviceIdType.MESH)

    own = [
        pltpu.make_async_copy(tok_hbm.at[of_wave(w), cols(b)], xs.at[w, b, t], local_sem.at[4])
        for w in range(WAVES)
    ]
    local = [
        pltpu.make_async_copy(tok_hbm, tok, local_sem.at[0]),
        pltpu.make_async_copy(wg_hbm, wg, local_sem.at[1]),
        pltpu.make_async_copy(wu_hbm, wu, local_sem.at[2]),
        pltpu.make_async_copy(wd_hbm, wd, local_sem.at[3]),
    ]
    notes = [
        pltpu.make_async_copy(ids_hbm, ids, local_sem.at[5]),
        pltpu.make_async_copy(values_hbm, values, local_sem.at[6]),
    ]
    barrier = pltpu.get_barrier_semaphore()
    signal(barrier, b, pair)
    signal(barrier, b, across)
    signal(barrier, blk(1), t)

    @pl.when(inner)
    def _():
        signal(barrier, blk(3), t)

    for copy in notes + local[:1] + own + local[1:]:
        copy.start()
    for copy in notes:
        copy.wait()
    meta[noted(b, t)] = jnp.zeros((SUBLANES, LANES), f32)
    meta[noted(b, t), 0:1, :all_rows] = ids[...].astype(f32)
    meta[noted(b, t), 1:2, :all_rows] = values[...]

    @pl.when(inner)
    def _():
        pl.semaphore_wait(barrier, 4)
        signal(far.at[0], blk(1), t)
        signal(far.at[0], blk(3), t)

    @pl.when(outer)
    def _():
        pl.semaphore_wait(barrier, 3)

    local[0].wait()
    arrived(fin_send.at[:, 0], local_sem.at[4])

    ready = set()

    def once(*name):
        if name in ready:
            return False
        ready.add(name)
        return True

    def only(side):
        def call(step):
            if side in ready:
                step()
        return call

    def announced(k):
        if k == 2 and once("far"):
            pl.semaphore_wait(far.at[0], 1)
            if "inner" in ready:
                signal(far.at[1], blk(1), t)
        if k == 3 and "outer" in ready and once("end"):
            pl.semaphore_wait(far.at[1], 1)

    def launch(w, k):
        announced(k)
        if once("launch", k):
            note = meta.at[noted(b, t)]
            remote(note, note, 9, m_recv.at[0, k], blk(k), t)
        remote(tok.at[of_wave(w), cols(blk(k))], xs.at[w, b, t], 0, z_recv.at[w, k - 1], blk(k), t)

    def spread(w, k):
        source = blk(k)
        mine = xs.at[w, source, t]
        if once("spread", k):
            note = meta.at[noted(source, t)]
            if k:
                arrived(note, m_recv.at[0, k])
            remote(note, note, 9, m_recv.at[1, k], b, across)
            remote(note, note, 9, m_recv.at[2, k], b, pair)
        if k:
            arrived(mine, z_recv.at[w, k - 1])
        remote(mine, mine, 1, x_recv.at[w, k], b, across)
        remote(mine, mine, 2, c_recv.at[w, k], b, pair)

    def pass_on(w, k):
        source = blk(k)
        theirs = xs.at[w, source, across]
        if once("pass", k):
            note = meta.at[noted(source, across)]
            arrived(note, m_recv.at[1, k])
            remote(note, note, 9, m_recv.at[2, k], b, pair)
        arrived(theirs, x_recv.at[w, k])
        remote(theirs, theirs, 2, c_recv.at[w, k], b, pair)

    def wide(mask, size):
        return jnp.concatenate([mask] * (size // LANES), axis=1)

    def prepare(k):
        source = blk(k)
        arrived(meta.at[pl.ds(0, 2)], m_recv.at[2, k])
        turned = jnp.transpose(meta[pl.ds(source * nt, nt)].reshape(nt * SUBLANES, LANES))
        for row, out in ((0, routes),) if k else ((0, routes), (1, scales)):
            for w in range(WAVES):
                column = jnp.concatenate(
                    [turned[w * rows:(w + 1) * rows, SUBLANES * i + row:SUBLANES * i + row + 1] for i in range(nt)],
                    axis=0,
                )
                out[w, k] = jnp.broadcast_to(column, (block, LANES))

    def contract(w, k):
        source = blk(k)
        if once("note", k):
            prepare(k)
        arrived(xs.at[w, source, pl.ds(0, 2)], c_recv.at[w, k])
        if once("up"):
            local[1].wait()
            local[2].wait()
        chosen = wide(routes[w, k], ff)
        x = xs[w, source].reshape(block, width)
        for at, weights in ((0, wg), (ff, wu)):
            total = None
            for e in range(experts):
                value = jnp.dot(x, weights[e], preferred_element_type=f32)
                total = value if e == 0 else jnp.where(chosen == e, value, total)
            part[w, k, :, at:at + ff] = total
            if k:
                part_send[w, k, :, at:at + ff] = total.astype(bf16)
        if k == 1:
            remote(part_send.at[w, 1], part_recv.at[w, 0], 6, p_recv.at[w, 0], blk(1), t)
        elif k:
            @only("outer")
            def _():
                remote(part_send.at[w, k], part_recv.at[w, 5 - k], 6, p_recv.at[w, 5 - k], blk(1), t)

    def relay(w, k):
        @only("inner")
        def _():
            arrived(part_recv.at[w, k], p_recv.at[w, k])
            part_send[w, k] = (part[w, k] + part_recv[w, k].astype(f32)).astype(bf16)
            remote(part_send.at[w, k], part_recv.at[w, 1], 6, p_recv.at[w, 1], blk(k), t)

    def activate(w, k):
        total = part[w, 0]
        for slot in (0, 1):
            arrived(part_recv.at[w, slot], p_recv.at[w, slot])
            total = total + part_recv[w, slot].astype(f32)
        gate, up = total[:, :ff], total[:, ff:]
        hid[w, b] = (gate / (1.0 + jnp.exp(-gate)) * up * wide(scales[w, 0], ff)).astype(bf16)
        mine = hid.at[w, b]

        @only("inner")
        def _():
            remote(mine, mine, 7, h_recv.at[w, 2], blk(3), t)

        remote(mine, mine, 7, h_recv.at[w, 0], blk(1), t)

    def forward(w, k):
        @only("inner")
        def _():
            source = blk(k)
            theirs = hid.at[w, source]
            arrived(theirs, h_recv.at[w, k - 1])
            if k == 1:
                remote(theirs, theirs, 8, h_recv.at[w, 1], blk(3), t)
            else:
                remote(theirs, theirs, 8, h_recv.at[w, 4 - k], blk(1), t)

    def expand(w, k):
        source = blk(k)
        if once("down"):
            local[3].wait()
        if k:
            if k in (1, 2, 3):
                @only("outer")
                def _():
                    arrived(hid.at[w, source], h_recv.at[w, k - 1])
            else:
                arrived(hid.at[w, source], h_recv.at[w, k - 1])
        chosen = wide(routes[w, k], ff)
        h = hid[w, source].astype(f32)
        routed = jnp.concatenate([jnp.where(chosen == e, h, 0.0).astype(bf16) for e in range(experts)], axis=1)
        ys[w, k] = jnp.dot(routed, wd[...].reshape(experts * ff, width), preferred_element_type=f32)
        for j, place in ((1, across_pair), (0, pair)):
            remote(ys.at[w, k, owned(place)], ycore.at[w, k, j], 3, y_recv.at[w, k], b, pair)

    def exchange(w, k):
        arrived(ycore.at[w, k], y_recv.at[w, k])
        yx_send[w, k] = (ys[w, k, owned(across), :] + ycore[w, k, 1]).astype(bf16)
        remote(yx_send.at[w, k], yx_recv.at[w, k], 4, yx_sem.at[w, k], b, across)

    def finish(w, k):
        total = ys[w, k, owned(t), :] + ycore[w, k, 0]
        arrived(yx_recv.at[w, k], yx_sem.at[w, k])
        total = total + yx_recv[w, k].astype(f32)
        if k:
            fin_send[w, k] = total.astype(bf16)
            remote(fin_send.at[w, k], out_ref.at[of_wave(w), cols(b)], 5, o_recv.at[0], blk(k), t)
        else:
            out_ref[of_wave(w), cols(b)] = total.astype(bf16)

    steps = {
        "Z": launch, "S": spread, "P": pass_on, "C": contract, "R": relay,
        "A": activate, "H": forward, "E": expand, "X": exchange, "F": finish,
    }
    def run(side, order):
        ready.clear()
        ready.add(side)
        for name, w, k in order:
            if side == "inner" and name != "Z" and (name, k) != ("S", 0):
                announced(2)
            steps[name](w, k)
        others = fin_send.at[:, pl.ds(1, nb - 1)]
        arrived(others, o_recv.at[0])
        for kind, ref in (
            (0, others), (1, yx_send), (2, xs.at[:, :, pl.ds(0, 2)]), (3, ycore), (4, yx_send), (5, others),
            (6, part_send.at[:, pl.ds(1, nb - 1)]), (9, meta.at[pl.ds(0, nb * nt - 1)]),
        ):
            arrived(ref, send_sem.at[kind])

        @only("inner")
        def _():
            arrived(hid.at[:, pl.ds(0, 2)], send_sem.at[7])
            arrived(hid.at[:, pl.ds(0, 3)], send_sem.at[8])

        @only("outer")
        def _():
            arrived(hid.at[:, pl.ds(0, 1)], send_sem.at[7])

    @pl.when(inner)
    def _():
        run("inner", INNER_ORDER)

    @pl.when(outer)
    def _():
        run("outer", OUTER_ORDER)


def stationary_body(nb, nt, tokens, expert_ids, gate_values, w_gate, w_up, w_down):
    rows, features = tokens.shape
    experts, width, ff = w_gate.shape
    f32, bf16 = jnp.float32, jnp.bfloat16
    wave_rows = rows // WAVES
    block = nt * wave_rows
    dma = pltpu.SemaphoreType.DMA
    hbm = pl.BlockSpec(memory_space=pltpu.HBM)
    each = (WAVES, nb)
    return pl.pallas_call(
        functools.partial(kernel, nb, nt),
        out_shape=pltpu.VMEM((rows, features), bf16),
        in_specs=[hbm] * 6,
        out_specs=pl.BlockSpec(memory_space=pltpu.VMEM),
        scratch_shapes=[
            pltpu.VMEM((rows, features), bf16),
            pltpu.VMEM((1, rows), jnp.int32),
            pltpu.VMEM((1, rows), f32),
            pltpu.VMEM((nb * nt, SUBLANES, LANES), f32),
            pltpu.VMEM(w_gate.shape, bf16),
            pltpu.VMEM(w_up.shape, bf16),
            pltpu.VMEM(w_down.shape, bf16),
            pltpu.VMEM((*each, block, LANES), f32),
            pltpu.VMEM((WAVES, 1, block, LANES), f32),
            pltpu.VMEM((*each, nt, wave_rows, width), bf16),
            pltpu.VMEM((*each, block, 2 * ff), f32),
            pltpu.VMEM((*each, block, 2 * ff), bf16),
            pltpu.VMEM((*each, block, 2 * ff), bf16),
            pltpu.VMEM((*each, block, ff), bf16),
            pltpu.VMEM((*each, block, width), f32),
            pltpu.VMEM((*each, 2, wave_rows, width), f32),
            pltpu.VMEM((*each, wave_rows, width), bf16),
            pltpu.VMEM((*each, wave_rows, width), bf16),
            pltpu.VMEM((*each, wave_rows, width), bf16),
            dma((7,)),
            dma((10,)),
            pltpu.SemaphoreType.REGULAR((2,)),
            dma((3, nb)),
            dma((WAVES, nb - 1)), dma(each), dma(each), dma(each), dma((WAVES, nb - 1)), dma(each), dma(each), dma((1,)),
        ],
        compiler_params=pltpu.CompilerParams(
            collective_id=0, has_side_effects=True, vmem_limit_bytes=60_000_000,
        ),
    )(tokens, expert_ids.reshape(1, rows), gate_values.reshape(1, rows), w_gate, w_up, w_down)


def solution(mesh):
    nb, nt = mesh.shape["blk"], mesh.shape["tok"]

    def body(tokens, expert_ids, gate_values, w_gate, w_up, w_down):
        rows = tokens.shape[0]
        width, ff = w_gate.shape[1], w_gate.shape[2]
        fits = width % LANES == 0 and ff % LANES == 0 and rows % (16 * WAVES) == 0 and rows <= LANES
        if fits and nt == 4 and nb == 4:
            return stationary_body(nb, nt, tokens, expert_ids, gate_values, w_gate, w_up, w_down)
        return gathered_body(tokens, expert_ids, gate_values, w_gate, w_up, w_down)

    return jax.shard_map(
        body,
        mesh=mesh,
        in_specs=(
            P(("groups", "blk", "tok"), None),
            P(("groups", "blk", "tok"), None),
            P(("groups", "blk", "tok"), None),
            P(None, "blk", "tok"),
            P(None, "blk", "tok"),
            P(None, "tok", "blk"),
        ),
        out_specs=P(("groups", "blk", "tok"), None),
        check_vma=False,
    )
```

```python
import functools

import jax
import jax.numpy as jnp
from jax import lax
from jax.experimental import pallas as pl
from jax.experimental.pallas import tpu as pltpu
from jax.sharding import PartitionSpec as P

LANES = 128
SUBLANES = 8
WAVES = 4
OUTER_ORDER = (
    ("S", 2, 0), ("S", 0, 0), ("Z", 0, 1), ("Z", 1, 1), ("Z", 2, 1), ("S", 3, 0), ("S", 1, 0),
    ("Z", 3, 1), ("Z", 3, 3), ("Z", 0, 3), ("Z", 2, 3), ("Z", 1, 3), ("P", 2, 0), ("S", 2, 1),
    ("P", 0, 0), ("C", 2, 0), ("Z", 3, 2), ("P", 3, 0), ("C", 0, 0), ("S", 1, 2), ("Z", 0, 2),
    ("P", 1, 0), ("C", 3, 0), ("S", 3, 2), ("Z", 2, 2), ("Z", 1, 2), ("C", 1, 0), ("P", 2, 1),
    ("S", 3, 3), ("C", 2, 1), ("S", 0, 3), ("P", 1, 2), ("S", 2, 3), ("S", 1, 3), ("P", 3, 2),
    ("C", 1, 2), ("S", 2, 2), ("S", 3, 1), ("C", 3, 2), ("P", 3, 3), ("P", 0, 3), ("C", 3, 3),
    ("P", 2, 3), ("C", 0, 3), ("P", 1, 3), ("P", 2, 2), ("C", 2, 3), ("S", 1, 1), ("P", 3, 1),
    ("C", 1, 3), ("C", 2, 2), ("C", 3, 1), ("S", 0, 2), ("P", 1, 1), ("C", 1, 1), ("P", 0, 2),
    ("S", 0, 1), ("C", 0, 2), ("A", 3, 0), ("E", 3, 0), ("P", 0, 1), ("A", 0, 0), ("X", 3, 0),
    ("E", 0, 0), ("C", 0, 1), ("A", 2, 0), ("E", 2, 0), ("X", 0, 0), ("A", 1, 0), ("E", 1, 0),
    ("X", 2, 0), ("F", 3, 0), ("E", 3, 1), ("X", 1, 0), ("X", 3, 1), ("E", 1, 1), ("X", 1, 1),
    ("F", 2, 0), ("E", 2, 1), ("E", 3, 2), ("X", 2, 1), ("F", 3, 1), ("E", 1, 2), ("X", 3, 2),
    ("F", 1, 1), ("X", 1, 2), ("E", 0, 1), ("E", 2, 2), ("F", 2, 1), ("X", 0, 1), ("E", 3, 3),
    ("F", 3, 2), ("X", 2, 2), ("E", 0, 3), ("F", 1, 2), ("X", 3, 3), ("E", 2, 3), ("X", 0, 3),
    ("E", 1, 3), ("X", 2, 3), ("F", 0, 0), ("E", 0, 2), ("F", 0, 1), ("X", 1, 3), ("F", 1, 0),
    ("F", 2, 2), ("X", 0, 2), ("F", 3, 3), ("F", 0, 3), ("F", 2, 3), ("F", 1, 3), ("F", 0, 2),
)
INNER_ORDER = (
    ("S", 1, 0), ("Z", 1, 3), ("S", 3, 0), ("Z", 3, 3), ("S", 0, 0), ("Z", 2, 1), ("S", 2, 0),
    ("Z", 1, 2), ("Z", 3, 2), ("P", 1, 0), ("S", 1, 3), ("S", 0, 1), ("P", 3, 0), ("S", 3, 3),
    ("S", 1, 1), ("C", 1, 0), ("S", 2, 1), ("P", 0, 0), ("C", 3, 0), ("Z", 2, 2), ("P", 2, 0),
    ("S", 3, 1), ("C", 0, 0), ("C", 2, 0), ("Z", 3, 1), ("P", 1, 3), ("P", 0, 1), ("C", 1, 3),
    ("P", 3, 3), ("C", 0, 1), ("Z", 0, 3), ("P", 1, 1), ("Z", 1, 1), ("P", 2, 1), ("C", 3, 3),
    ("Z", 2, 3), ("S", 3, 2), ("P", 3, 1), ("C", 1, 1), ("C", 2, 1), ("Z", 0, 2), ("S", 0, 2),
    ("C", 3, 1), ("S", 2, 2), ("S", 1, 2), ("S", 0, 3), ("S", 2, 3), ("P", 3, 2), ("C", 3, 2),
    ("R", 1, 3), ("P", 0, 2), ("P", 2, 2), ("P", 1, 2), ("C", 0, 2), ("R", 3, 3), ("P", 0, 3),
    ("C", 2, 2), ("Z", 0, 1), ("C", 1, 2), ("P", 2, 3), ("R", 3, 2), ("C", 0, 3), ("C", 2, 3),
    ("R", 0, 2), ("R", 2, 2), ("R", 1, 2), ("R", 2, 3), ("A", 3, 0), ("E", 3, 0), ("A", 1, 0),
    ("E", 1, 0), ("X", 3, 0), ("R", 0, 3), ("X", 1, 0), ("A", 2, 0), ("E", 2, 0), ("H", 3, 1),
    ("E", 3, 1), ("H", 3, 3), ("E", 3, 3), ("H", 0, 1), ("E", 0, 1), ("X", 2, 0), ("X", 3, 1),
    ("H", 1, 3), ("E", 1, 3), ("X", 3, 3), ("F", 3, 0), ("X", 0, 1), ("H", 2, 1), ("E", 2, 1),
    ("X", 1, 3), ("F", 1, 0), ("H", 1, 1), ("E", 1, 1), ("A", 0, 0), ("E", 0, 0), ("X", 2, 1),
    ("H", 2, 3), ("E", 2, 3), ("X", 1, 1), ("F", 2, 0), ("H", 3, 2), ("E", 3, 2), ("X", 0, 0),
    ("F", 3, 1), ("X", 2, 3), ("H", 0, 2), ("E", 0, 2), ("F", 3, 3), ("X", 3, 2), ("H", 2, 2),
    ("E", 2, 2), ("X", 0, 2), ("H", 1, 2), ("E", 1, 2), ("F", 1, 3), ("X", 2, 2), ("H", 0, 3),
    ("F", 2, 1), ("E", 0, 3), ("F", 0, 1), ("F", 1, 1), ("X", 1, 2), ("F", 0, 0), ("X", 0, 3),
    ("F", 2, 3), ("F", 3, 2), ("F", 0, 2), ("F", 2, 2), ("F", 1, 2), ("F", 0, 3),
)


def gathered_body(tokens, expert_ids, gate_values, w_gate, w_up, w_down):
    group_rows = lax.all_gather(tokens, "tok", axis=0, tiled=True)
    group_routes = lax.all_gather(expert_ids, "tok", axis=0, tiled=True)[:, 0]
    experts = w_gate.shape[0]
    count_rows = group_rows.shape[0]
    capacity = 3 * count_rows // 4
    expert_range = jnp.arange(experts, dtype=jnp.int32)
    onehot = (group_routes[:, None] == expert_range[None, :]).astype(jnp.int32)
    slot_rank = jnp.sum((jnp.cumsum(onehot, axis=0) - onehot) * onehot, axis=1)
    expert_match = group_routes[None, None, :] == expert_range[:, None, None]
    slot_match = slot_rank[None, None, :] == jnp.arange(capacity, dtype=jnp.int32)[None, :, None]
    dispatch = (expert_match & slot_match).astype(jnp.bfloat16)
    slots = jnp.einsum(
        "esg,gd->esd", dispatch, group_rows, preferred_element_type=jnp.float32
    ).astype(jnp.bfloat16)

    def add_part(weights):
        return jnp.einsum("esd,edf->esf", slots, weights, preferred_element_type=jnp.float32)

    gate_sum = add_part(lax.all_gather(w_gate, "blk", axis=1, tiled=True))
    up_sum = add_part(lax.all_gather(w_up, "blk", axis=1, tiled=True))
    hidden = (jax.nn.silu(gate_sum) * up_sum).astype(jnp.bfloat16)
    slot_out = jnp.einsum(
        "esf,efd->esd",
        hidden,
        lax.all_gather(w_down, "blk", axis=2, tiled=True),
        preferred_element_type=jnp.float32,
    )
    flat_rows = slot_out.reshape(experts * capacity, slot_out.shape[2])
    position = group_routes * capacity + slot_rank
    partial_value = jnp.take(flat_rows, position, axis=0)
    summed = lax.psum_scatter(partial_value, "tok", scatter_dimension=0, tiled=True)
    return (gate_values * summed).astype(jnp.bfloat16)


def kernel(
    nb, nt, tok_hbm, ids_hbm, values_hbm, wg_hbm, wu_hbm, wd_hbm, out_ref,
    tok, ids, values, meta, wg, wu, wd, routes, scales, xs, part, part_send, part_recv, hid, ys, ycore,
    yx_send, yx_recv, fin_send,
    local_sem, send_sem, far, m_recv, z_recv, x_recv, c_recv, p_recv, h_recv, y_recv, yx_sem, o_recv,
):
    g, b, t = lax.axis_index("groups"), lax.axis_index("blk"), lax.axis_index("tok")
    all_rows, width = tok.shape[0], xs.shape[4]
    rows = all_rows // WAVES
    block = nt * rows
    experts, ff = wg.shape[0], wg.shape[2]
    f32, bf16 = jnp.float32, jnp.bfloat16
    pair = t + 1 - 2 * lax.rem(t, 2)
    across = lax.rem(t + 2, nt)
    across_pair = lax.rem(pair + 2, nt)
    outer = lax.rem((b + 1) // 2 + 1, 2) == 1
    inner = jnp.logical_not(outer)

    low, high = lax.rem(b, 2), b // 2
    blocks = [b, 2 * high + 1 - low, 2 * (1 - high) + low, 2 * (1 - high) + 1 - low]

    def blk(k):
        return blocks[k]

    def cols(index):
        return pl.ds(pl.multiple_of(index * width, LANES), width)

    def of_wave(w):
        return pl.ds(w * rows, rows)

    def noted(block_at, token_at):
        return block_at * nt + token_at

    def owned(index):
        return pl.ds(pl.multiple_of(index * rows, SUBLANES), rows)

    def remote(src, dst, kind, recv, to_b, to_t):
        pltpu.make_async_remote_copy(
            src_ref=src, dst_ref=dst, send_sem=send_sem.at[kind], recv_sem=recv,
            device_id=(g, to_b, to_t), device_id_type=pl.DeviceIdType.MESH,
        ).start()

    def arrived(dst, recv):
        pltpu.make_async_copy(dst, dst, recv).wait()

    def signal(sem, to_b, to_t):
        pl.semaphore_signal(sem, inc=1, device_id=(g, to_b, to_t), device_id_type=pl.DeviceIdType.MESH)

    own = [
        pltpu.make_async_copy(tok_hbm.at[of_wave(w), cols(b)], xs.at[w, b, t], local_sem.at[4])
        for w in range(WAVES)
    ]
    local = [
        pltpu.make_async_copy(tok_hbm, tok, local_sem.at[0]),
        pltpu.make_async_copy(wg_hbm, wg, local_sem.at[1]),
        pltpu.make_async_copy(wu_hbm, wu, local_sem.at[2]),
        pltpu.make_async_copy(wd_hbm, wd, local_sem.at[3]),
    ]
    notes = [
        pltpu.make_async_copy(ids_hbm, ids, local_sem.at[5]),
        pltpu.make_async_copy(values_hbm, values, local_sem.at[6]),
    ]
    barrier = pltpu.get_barrier_semaphore()
    signal(barrier, b, pair)
    signal(barrier, b, across)
    signal(barrier, blk(1), t)

    @pl.when(inner)
    def _():
        signal(barrier, blk(3), t)

    for copy in notes + local[:1] + own + local[1:]:
        copy.start()
    for copy in notes:
        copy.wait()
    meta[noted(b, t)] = jnp.zeros((SUBLANES, LANES), f32)
    meta[noted(b, t), 0:1, :all_rows] = ids[...].astype(f32)
    meta[noted(b, t), 1:2, :all_rows] = values[...]

    @pl.when(inner)
    def _():
        pl.semaphore_wait(barrier, 4)
        signal(far.at[0], blk(1), t)
        signal(far.at[0], blk(3), t)

    @pl.when(outer)
    def _():
        pl.semaphore_wait(barrier, 3)

    local[0].wait()
    arrived(fin_send.at[:, 0], local_sem.at[4])

    ready = set()

    def once(*name):
        if name in ready:
            return False
        ready.add(name)
        return True

    def only(side):
        def call(step):
            if side in ready:
                step()
        return call

    def announced(k):
        if k == 2 and once("far"):
            pl.semaphore_wait(far.at[0], 1)
            if "inner" in ready:
                signal(far.at[1], blk(1), t)
        if k == 3 and "outer" in ready and once("end"):
            pl.semaphore_wait(far.at[1], 1)

    def launch(w, k):
        announced(k)
        if once("launch", k):
            note = meta.at[noted(b, t)]
            remote(note, note, 9, m_recv.at[0, k], blk(k), t)
        remote(tok.at[of_wave(w), cols(blk(k))], xs.at[w, b, t], 0, z_recv.at[w, k - 1], blk(k), t)

    def spread(w, k):
        source = blk(k)
        mine = xs.at[w, source, t]
        if once("spread", k):
            note = meta.at[noted(source, t)]
            if k:
                arrived(note, m_recv.at[0, k])
            remote(note, note, 9, m_recv.at[1, k], b, across)
            remote(note, note, 9, m_recv.at[2, k], b, pair)
        if k:
            arrived(mine, z_recv.at[w, k - 1])
        remote(mine, mine, 1, x_recv.at[w, k], b, across)
        remote(mine, mine, 2, c_recv.at[w, k], b, pair)

    def pass_on(w, k):
        source = blk(k)
        theirs = xs.at[w, source, across]
        if once("pass", k):
            note = meta.at[noted(source, across)]
            arrived(note, m_recv.at[1, k])
            remote(note, note, 9, m_recv.at[2, k], b, pair)
        arrived(theirs, x_recv.at[w, k])
        remote(theirs, theirs, 2, c_recv.at[w, k], b, pair)

    def wide(mask, size):
        return jnp.concatenate([mask] * (size // LANES), axis=1)

    def prepare(k):
        source = blk(k)
        arrived(meta.at[pl.ds(0, 2)], m_recv.at[2, k])
        turned = jnp.transpose(meta[pl.ds(source * nt, nt)].reshape(nt * SUBLANES, LANES))
        for row, out in ((0, routes),) if k else ((0, routes), (1, scales)):
            for w in range(WAVES):
                column = jnp.concatenate(
                    [turned[w * rows:(w + 1) * rows, SUBLANES * i + row:SUBLANES * i + row + 1] for i in range(nt)],
                    axis=0,
                )
                out[w, k] = jnp.broadcast_to(column, (block, LANES))

    def contract(w, k):
        source = blk(k)
        if once("note", k):
            prepare(k)
        arrived(xs.at[w, source, pl.ds(0, 2)], c_recv.at[w, k])
        if once("up"):
            local[1].wait()
            local[2].wait()
        chosen = wide(routes[w, k], ff)
        x = xs[w, source].reshape(block, width)
        for at, weights in ((0, wg), (ff, wu)):
            total = None
            for e in range(experts):
                value = jnp.dot(x, weights[e], preferred_element_type=f32)
                total = value if e == 0 else jnp.where(chosen == e, value, total)
            part[w, k, :, at:at + ff] = total
            if k:
                part_send[w, k, :, at:at + ff] = total.astype(bf16)
        if k == 1:
            remote(part_send.at[w, 1], part_recv.at[w, 0], 6, p_recv.at[w, 0], blk(1), t)
        elif k:
            @only("outer")
            def _():
                remote(part_send.at[w, k], part_recv.at[w, 5 - k], 6, p_recv.at[w, 5 - k], blk(1), t)

    def relay(w, k):
        @only("inner")
        def _():
            arrived(part_recv.at[w, k], p_recv.at[w, k])
            part_send[w, k] = (part[w, k] + part_recv[w, k].astype(f32)).astype(bf16)
            remote(part_send.at[w, k], part_recv.at[w, 1], 6, p_recv.at[w, 1], blk(k), t)

    def activate(w, k):
        total = part[w, 0]
        for slot in (0, 1):
            arrived(part_recv.at[w, slot], p_recv.at[w, slot])
            total = total + part_recv[w, slot].astype(f32)
        gate, up = total[:, :ff], total[:, ff:]
        hid[w, b] = (gate / (1.0 + jnp.exp(-gate)) * up * wide(scales[w, 0], ff)).astype(bf16)
        mine = hid.at[w, b]

        @only("inner")
        def _():
            remote(mine, mine, 7, h_recv.at[w, 2], blk(3), t)

        remote(mine, mine, 7, h_recv.at[w, 0], blk(1), t)

    def forward(w, k):
        @only("inner")
        def _():
            source = blk(k)
            theirs = hid.at[w, source]
            arrived(theirs, h_recv.at[w, k - 1])
            if k == 1:
                remote(theirs, theirs, 8, h_recv.at[w, 1], blk(3), t)
            else:
                remote(theirs, theirs, 8, h_recv.at[w, 4 - k], blk(1), t)

    def expand(w, k):
        source = blk(k)
        if once("down"):
            local[3].wait()
        if k:
            if k in (1, 2, 3):
                @only("outer")
                def _():
                    arrived(hid.at[w, source], h_recv.at[w, k - 1])
            else:
                arrived(hid.at[w, source], h_recv.at[w, k - 1])
        chosen = wide(routes[w, k], ff)
        h = hid[w, source].astype(f32)
        routed = jnp.concatenate([jnp.where(chosen == e, h, 0.0).astype(bf16) for e in range(experts)], axis=1)
        ys[w, k] = jnp.dot(routed, wd[...].reshape(experts * ff, width), preferred_element_type=f32)
        for j, place in ((1, across_pair), (0, pair)):
            remote(ys.at[w, k, owned(place)], ycore.at[w, k, j], 3, y_recv.at[w, k], b, pair)

    def exchange(w, k):
        arrived(ycore.at[w, k], y_recv.at[w, k])
        yx_send[w, k] = (ys[w, k, owned(across), :] + ycore[w, k, 1]).astype(bf16)
        remote(yx_send.at[w, k], yx_recv.at[w, k], 4, yx_sem.at[w, k], b, across)

    def finish(w, k):
        total = ys[w, k, owned(t), :] + ycore[w, k, 0]
        arrived(yx_recv.at[w, k], yx_sem.at[w, k])
        total = total + yx_recv[w, k].astype(f32)
        if k:
            fin_send[w, k] = total.astype(bf16)
            remote(fin_send.at[w, k], out_ref.at[of_wave(w), cols(b)], 5, o_recv.at[0], blk(k), t)
        else:
            out_ref[of_wave(w), cols(b)] = total.astype(bf16)

    steps = {
        "Z": launch, "S": spread, "P": pass_on, "C": contract, "R": relay,
        "A": activate, "H": forward, "E": expand, "X": exchange, "F": finish,
    }
    def run(side, order):
        ready.clear()
        ready.add(side)
        for name, w, k in order:
            if side == "inner" and name != "Z" and (name, k) != ("S", 0):
                announced(2)
            steps[name](w, k)
        others = fin_send.at[:, pl.ds(1, nb - 1)]
        arrived(others, o_recv.at[0])
        for kind, ref in (
            (0, others), (1, yx_send), (2, xs.at[:, :, pl.ds(0, 2)]), (3, ycore), (4, yx_send), (5, others),
            (6, part_send.at[:, pl.ds(1, nb - 1)]), (9, meta.at[pl.ds(0, nb * nt - 1)]),
        ):
            arrived(ref, send_sem.at[kind])

        @only("inner")
        def _():
            arrived(hid.at[:, pl.ds(0, 2)], send_sem.at[7])
            arrived(hid.at[:, pl.ds(0, 3)], send_sem.at[8])

        @only("outer")
        def _():
            arrived(hid.at[:, pl.ds(0, 1)], send_sem.at[7])

    @pl.when(inner)
    def _():
        run("inner", INNER_ORDER)

    @pl.when(outer)
    def _():
        run("outer", OUTER_ORDER)


def stationary_body(nb, nt, tokens, expert_ids, gate_values, w_gate, w_up, w_down):
    rows, features = tokens.shape
    experts, width, ff = w_gate.shape
    f32, bf16 = jnp.float32, jnp.bfloat16
    wave_rows = rows // WAVES
    block = nt * wave_rows
    dma = pltpu.SemaphoreType.DMA
    hbm = pl.BlockSpec(memory_space=pltpu.HBM)
    each = (WAVES, nb)
    return pl.pallas_call(
        functools.partial(kernel, nb, nt),
        out_shape=pltpu.VMEM((rows, features), bf16),
        in_specs=[hbm] * 6,
        out_specs=pl.BlockSpec(memory_space=pltpu.VMEM),
        scratch_shapes=[
            pltpu.VMEM((rows, features), bf16),
            pltpu.VMEM((1, rows), jnp.int32),
            pltpu.VMEM((1, rows), f32),
            pltpu.VMEM((nb * nt, SUBLANES, LANES), f32),
            pltpu.VMEM(w_gate.shape, bf16),
            pltpu.VMEM(w_up.shape, bf16),
            pltpu.VMEM(w_down.shape, bf16),
            pltpu.VMEM((*each, block, LANES), f32),
            pltpu.VMEM((WAVES, 1, block, LANES), f32),
            pltpu.VMEM((*each, nt, wave_rows, width), bf16),
            pltpu.VMEM((*each, block, 2 * ff), f32),
            pltpu.VMEM((*each, block, 2 * ff), bf16),
            pltpu.VMEM((*each, block, 2 * ff), bf16),
            pltpu.VMEM((*each, block, ff), bf16),
            pltpu.VMEM((*each, block, width), f32),
            pltpu.VMEM((*each, 2, wave_rows, width), f32),
            pltpu.VMEM((*each, wave_rows, width), bf16),
            pltpu.VMEM((*each, wave_rows, width), bf16),
            pltpu.VMEM((*each, wave_rows, width), bf16),
            dma((7,)),
            dma((10,)),
            pltpu.SemaphoreType.REGULAR((2,)),
            dma((3, nb)),
            dma((WAVES, nb - 1)), dma(each), dma(each), dma(each), dma((WAVES, nb - 1)), dma(each), dma(each), dma((1,)),
        ],
        compiler_params=pltpu.CompilerParams(
            collective_id=0, has_side_effects=True, vmem_limit_bytes=60_000_000,
        ),
    )(tokens, expert_ids.reshape(1, rows), gate_values.reshape(1, rows), w_gate, w_up, w_down)


def solution(mesh):
    nb, nt = mesh.shape["blk"], mesh.shape["tok"]

    def body(tokens, expert_ids, gate_values, w_gate, w_up, w_down):
        rows = tokens.shape[0]
        width, ff = w_gate.shape[1], w_gate.shape[2]
        fits = width % LANES == 0 and ff % LANES == 0 and rows % (16 * WAVES) == 0 and rows <= LANES
        if fits and nt == 4 and nb == 4:
            return stationary_body(nb, nt, tokens, expert_ids, gate_values, w_gate, w_up, w_down)
        return gathered_body(tokens, expert_ids, gate_values, w_gate, w_up, w_down)

    return jax.shard_map(
        body,
        mesh=mesh,
        in_specs=(
            P(("groups", "blk", "tok"), None),
            P(("groups", "blk", "tok"), None),
            P(("groups", "blk", "tok"), None),
            P(None, "blk", "tok"),
            P(None, "blk", "tok"),
            P(None, "tok", "blk"),
        ),
        out_specs=P(("groups", "blk", "tok"), None),
        check_vma=False,
    )
```
